256 devices in a mesh: groups: 4 (over y, x), row: 64 (over z, core).
Axes of the slice: x: 2, y: 2, z: 32, core: 2. Of those that a mesh axis runs over, the one named last changes fastest.
The devices are a block of a 4x8x32 slice.
Arguments:
- pair_in: bfloat16 [2048, 512, 128], P(('groups', 'row')), parts along dimension 0, may hold values from -6 to 6
- valid_tokens: int32 [2048], P('groups'), parts along dimension 0, may hold values 0 or 1
- proj_weight: bfloat16 [2, 128, 640], replicated, may hold values from -0.5 to 0.5
- out_weight: bfloat16 [2, 128, 128], replicated, may hold values from -0.5 to 0.5
- norm_gains: float32 [2, 2, 128], replicated, may hold values from 0.1 to 1.9
Outputs:
- pair_out: bfloat16 [2048, 512, 128], P(('groups', 'row')), parts along dimension 0
The draws below stay inside these ranges and needn't reach their ends.
There are 4 independent parts, one for each index of `groups`. The reference program is written for one: setup_inputs(seed, part) draws one part's arguments, and reference() takes and returns one part's arrays. A program takes and returns all parts, laid end to end along the dimension named above; an argument that names none is the same for every part. Nothing has to cross between parts.
All inputs are finite; a program needn't handle non-finite values.
Results may differ from the reference program's by a relative error of at most 0.007.
Values may be sent and summed in bfloat16 or wider, within the bound.
A program may use at most 64 MiB of HBM per device.

```python
import jax
import jax.numpy as jnp
from jax import lax

C = 128
N = 512


def touch_ends(result, stream_key, low, top_value):
    place = [jax.random.randint(jax.random.fold_in(stream_key, axis), (), 0, length) for axis, length in enumerate(result.shape)]
    main_axis = result.shape.index(max(result.shape))
    neighbour = place[:main_axis] + [(place[main_axis] + 1) % result.shape[main_axis]] + place[main_axis + 1:]
    return result.at[tuple(place)].set(low).at[tuple(neighbour)].set(top_value)


def steps_of(key, shape, split, low, top_value):
    def one(position, parts):
        heights = jax.random.uniform(jax.random.fold_in(jax.random.fold_in(key, 6), position), (parts,), jnp.float32, low / len(split), top_value / len(split))
        return jnp.repeat(jnp.exp(heights), shape[position] // parts).reshape((-1,) + (1,) * (len(shape) - position - 1))

    factor_of = one(*split[0])
    for cut in split[1:]:
        factor_of = factor_of * one(*cut)
    return factor_of


def gaussian(key, extent, scale, bound, split=(), dtype=jnp.bfloat16):
    array = jax.random.normal(key, extent, jnp.float32) * scale
    if len(split) > 0:
        array = steps_of(key, extent, split, -0.22, 0.18) * array
    return jnp.clip(array, min=-bound, max=bound).astype(dtype)


def setup_inputs(seed: int = 0, part: int = 0) -> dict:
    arg_keys = jax.random.split(jax.random.key(seed), 6)
    part_splits = jax.random.split(jax.random.fold_in(arg_keys[5], part), 6)
    pair_in = gaussian(part_splits[0], (N, N, C), 1.0, 6.0, ((0, 64),))
    valid_tokens = touch_ends((jax.random.randint(part_splits[1], (N,), 0, 8) < 7).astype(jnp.int32), jax.random.fold_in(part_splits[1], 1), 0, 1)
    proj_weight = gaussian(arg_keys[2], (2, C, 5 * C), C ** -0.5, 0.5)
    out_weight = gaussian(arg_keys[3], (2, C, C), C ** -0.5, 0.5)
    norm_gains = jnp.clip(1.0 + 0.18 * jax.random.normal(arg_keys[4], (2, 2, C), jnp.float32), 0.1, 1.9)
    return {"pair_in": pair_in, "valid_tokens": valid_tokens, "proj_weight": proj_weight, "out_weight": out_weight, "norm_gains": norm_gains}


EPSILON = 1e-05

def layer_norm(values, gain):
    mean = lax.optimization_barrier(jnp.mean(values, axis=-1, keepdims=True))
    centered = values - mean
    variance = lax.optimization_barrier(jnp.mean(centered * centered, axis=-1, keepdims=True))
    return centered * lax.rsqrt(variance + EPSILON) * gain

def one_update(pair, valid_tokens, proj, outw, gains, incoming):
    width = pair.shape[-1]
    count = pair.shape[0]
    normed = layer_norm(pair.astype(jnp.float32), gains[0]).astype(jnp.bfloat16)
    flat_rows = normed.reshape(count * count, width)
    projected = jnp.dot(flat_rows, proj, preferred_element_type=jnp.float32).reshape(count, count, 5 * width)
    valid = valid_tokens.astype(jnp.float32)
    mask = (valid[:, None] * valid[None, :])[:, :, None]
    left = (jax.nn.sigmoid(projected[..., 0:width]) * projected[..., width:2 * width] * mask).astype(jnp.bfloat16)
    right = (jax.nn.sigmoid(projected[..., 2 * width:3 * width]) * projected[..., 3 * width:4 * width] * mask).astype(jnp.bfloat16)
    gate_values = jax.nn.sigmoid(projected[..., 4 * width:])
    left_cf = jnp.transpose(left, (2, 0, 1)).astype(jnp.float32)
    right_cf = jnp.transpose(right, (2, 0, 1)).astype(jnp.float32)
    if incoming:
        triangle = jnp.einsum('cki,ckj->cij', left_cf, right_cf)
    else:
        triangle = jnp.einsum('cik,cjk->cij', left_cf, right_cf)
    triangle = jnp.transpose(triangle.astype(jnp.bfloat16), (1, 2, 0)).astype(jnp.float32)
    output_normed = layer_norm(triangle, gains[1]).astype(jnp.bfloat16)
    update_rows = jnp.dot(output_normed.reshape(count * count, width), outw, preferred_element_type=jnp.float32)
    update_rows = update_rows.reshape(count, count, width) * gate_values
    return (pair.astype(jnp.float32) + update_rows).astype(jnp.bfloat16)

def reference(pair_in, valid_tokens, proj_weight, out_weight, norm_gains):
    middle = one_update(pair_in, valid_tokens, proj_weight[0], out_weight[0], norm_gains[0], False)
    return one_update(middle, valid_tokens, proj_weight[1], out_weight[1], norm_gains[1], True)
```

```python
import functools

import jax
import jax.numpy as jnp
from jax import lax
from jax.experimental import pallas as pl
from jax.experimental.pallas import tpu as pltpu
from jax.sharding import PartitionSpec as P

MESH = pl.DeviceIdType.MESH
EPSILON = 1e-05
SPREAD = 7
LANES = 128
BF16 = jnp.bfloat16
F32 = jnp.float32


def dot(a, b, contract_a, contract_b):
    return lax.dot_general(
        a, b, (((contract_a,), (contract_b,)), ((), ())), preferred_element_type=F32
    )


def kernel(
    peers,
    pair_ref,
    mask_ref,
    wt_ref,
    wg_ref,
    wo_ref,
    gin_ref,
    gout_ref,
    out_ref,
    left_f,
    right_f,
    tri_f,
    normed,
    gates,
    middle,
    src0,
    src1,
    land_l0,
    land_r0,
    land_l1,
    land_r1,
    mat_l,
    mat_r,
    part,
    tri_out0,
    tri_out1,
    tri_in0,
    tri_in1,
    swap_out,
    swap_in,
    scat_send,
    scat_recv0,
    scat_recv1,
    swap_send,
    swap_recv,
    tri_send,
    tri_recv,
):
    rows, count, width = pair_ref.shape
    chips = peers // 2
    half = chips // 2
    inner = (SPREAD + 1) // 2
    outer = half - inner
    cols = count // 2
    blocks_per_half = cols // LANES
    me = lax.axis_index("row")
    chip = me // 2
    core = me % 2
    other = 1 - core

    def wrap(a):
        return lax.rem(a + 4 * chips, chips)

    def device(at_chip, at_core):
        return {"row": wrap(at_chip) * 2 + at_core}

    def send(src, dst, ssem, rsem, at_chip, at_core):
        pltpu.make_async_remote_copy(
            src_ref=src,
            dst_ref=dst,
            send_sem=ssem,
            recv_sem=rsem,
            device_id=device(at_chip, at_core),
            device_id_type=MESH,
        ).start()

    def waiter(ref, ssem, rsem):
        return pltpu.make_async_remote_copy(
            src_ref=ref,
            dst_ref=ref,
            send_sem=ssem,
            recv_sem=rsem,
            device_id=device(chip, other),
            device_id_type=MESH,
        )

    def role_of(chunk):
        return lax.rem(chip + chunk, 2)

    def owned_set(role):
        return wrap(chip - SPREAD * role)

    def base_of(role):
        return (chips - outer) + role * (inner - (chips - outer))

    def self_slot(role):
        return outer + role * (SPREAD - inner - outer)

    barrier = pltpu.get_barrier_semaphore()
    reach = 2 * outer + 1

    def greet(i, carry):
        at = chip - outer + i
        pl.semaphore_signal(
            barrier, inc=1, device_id=device(at, other), device_id_type=MESH
        )

        @pl.when(i != outer)
        def _():
            pl.semaphore_signal(
                barrier, inc=1, device_id=device(at, core), device_id_type=MESH
            )

        return carry

    lax.fori_loop(0, reach, greet, 0)

    def project(u, h, pair):
        span = pl.ds(h * cols, cols)

        def row(r, carry):
            z = pair[r, span, :].astype(F32)
            mean = jnp.mean(z, axis=1, keepdims=True)
            centered = z - mean
            var = jnp.mean(centered * centered, axis=1, keepdims=True)
            x = (centered * lax.rsqrt(var + EPSILON) * gin_ref[u]).astype(BF16)
            normed[r, span, :] = x
            m = mask_ref[pl.ds(r, 1), span]
            for k, store in ((2, right_f), (0, left_f)):
                gate = dot(wt_ref[u, k * width : (k + 1) * width, :], x, 1, 1)
                value = dot(wt_ref[u, (k + 1) * width : (k + 2) * width, :], x, 1, 1)
                edge = jax.nn.sigmoid(gate) * value * m
                for b in range(blocks_per_half):
                    store[h * blocks_per_half + b, pl.ds(r, width, stride=rows), :] = edge[
                        :, b * LANES : (b + 1) * LANES
                    ]
            return carry

        lax.fori_loop(0, rows, row, 0)

    def gate_values(u):
        def row(r, carry):
            gates[r] = jax.nn.sigmoid(dot(normed[r], wg_ref[u], 1, 0))
            return carry

        lax.fori_loop(0, rows, row, 0)

    tile = 2 * rows

    def packed(store, at, first, number):
        return jnp.concatenate(
            [store[first + b, at, :] for b in range(number)], axis=1
        ).astype(BF16)

    def finish(u, h, pair, result, tri_in):
        span = pl.ds(h * cols, cols)

        def unpack(p, carry):
            at = pl.ds(pl.multiple_of(p * tile, tile), tile)
            block = tri_in[h, p].astype(F32)
            for b in range(blocks_per_half):
                tri_f[b, at, :] = block[:, b * LANES : (b + 1) * LANES]
            return carry

        lax.fori_loop(0, peers, unpack, 0, unroll=4)

        def row(r, carry):
            t = jnp.concatenate(
                [tri_f[b, pl.ds(r, width, stride=rows), :] for b in range(blocks_per_half)], axis=1
            )
            mean = jnp.mean(t, axis=0, keepdims=True)
            centered = t - mean
            var = jnp.mean(centered * centered, axis=0, keepdims=True)
            y = (centered * lax.rsqrt(var + EPSILON) * gout_ref[u]).astype(BF16)
            update = dot(y, wo_ref[u], 0, 0)
            z = pair[r, span, :].astype(F32)
            result[r, span, :] = (z + update * gates[r, span, :]).astype(BF16)
            return carry

        lax.fori_loop(0, rows, row, 0)

    def scatter(chunk, items):
        odd = lax.rem(chip + chunk, 2)

        def step(k, carry):
            for role in range(2):
                if role == 0:
                    ahead = outer - odd - 2 * k
                    t = wrap(-ahead)
                    slot = odd + 2 * k
                else:
                    ahead = 2 * k - odd - (outer - 1)
                    t = SPREAD - ahead
                    slot = t - inner
                home = wrap(chip - t)
                for src, dst_of, ssem, rsem in items:
                    send(
                        src.at[home * 2 + other],
                        dst_of(role, slot * 2 + core),
                        ssem,
                        rsem(role),
                        chip + ahead,
                        other,
                    )

                    @pl.when(ahead != 0)
                    def _():
                        send(
                            src.at[home * 2 + core],
                            dst_of(role, slot * 2 + core),
                            ssem,
                            rsem(role),
                            chip + ahead,
                            core,
                        )

                    @pl.when(ahead == 0)
                    def _():
                        dst_of(role, slot * 2 + core)[...] = src[home * 2 + core]

            return carry

        lax.fori_loop(0, half // 2, step, 0)

    def return_tri(role, h, tri_out, tri_in, ssem, rsem):
        home = owned_set(role)
        base = base_of(role)
        own = self_slot(role)
        pair_index = home * 2 + core

        def step(i, carry):
            k = i + role * (half - 1 - 2 * i)
            at = home + base + k
            send(
                tri_out.at[role, h, 2 * k + other],
                tri_in.at[h, pair_index],
                ssem,
                rsem,
                at,
                other,
            )

            @pl.when(k != own)
            def _():
                send(
                    tri_out.at[role, h, 2 * k + core],
                    tri_in.at[h, pair_index],
                    ssem,
                    rsem,
                    at,
                    core,
                )

            @pl.when(k == own)
            def _():
                tri_in[h, pair_index] = tri_out[role, h, 2 * k + core]

            return carry

        lax.fori_loop(0, half, step, 0)

    for h in range(2):
        project(0, h, pair_ref)

    def pack0(p, carry):
        at = pl.ds(pl.multiple_of(p * tile, tile), tile)
        src0[0, p] = packed(right_f, at, 0, 2 * blocks_per_half)
        src0[1, p] = packed(left_f, at, 0, 2 * blocks_per_half)
        return carry

    lax.fori_loop(0, peers, pack0, 0, unroll=2)

    pl.semaphore_wait(barrier, 2 * reach - 1)

    def natural(role, slot_core):
        return land_r0.at[role, me]

    def slotted(role, slot_core):
        return land_l0.at[role, slot_core]

    for chunk in range(2):
        scatter(chunk, [(src0.at[0], natural, scat_send.at[0, chunk], lambda r: scat_recv0.at[0, r])])
        scatter(chunk, [(src0.at[1], slotted, scat_send.at[1, chunk], lambda r: scat_recv0.at[1, r])])

    gate_values(0)

    for chunk in range(2):
        role = role_of(chunk)
        home = owned_set(role)
        base = base_of(role)
        first = land_r0.at[role, pl.ds(0, peers // 2 - 1)]
        waiter(first, scat_send.at[0, 0], scat_recv0.at[0, role]).wait_recv()

        def pass_on(k, carry):
            at = wrap(home + base + k) * 2
            send(
                land_r0.at[role, pl.ds(at, 2)],
                land_r0.at[1 - role, pl.ds(at, 2)],
                swap_send.at[0, chunk],
                swap_recv.at[0, 1 - role],
                chip + SPREAD - 2 * SPREAD * role,
                core,
            )
            return carry

        lax.fori_loop(0, half, pass_on, 0)

    def multiply0(role):
        def split_r(s, carry):
            block = land_r0[role, pl.ds(2 * s, 2)].astype(F32)
            block = block.reshape(2, 2, rows, count)
            at = pl.ds(pl.multiple_of(s * tile, tile), tile)
            for e in range(2):
                mat_r[e, at, :] = block[:, e].reshape(tile, count).astype(BF16)
            return carry

        lax.fori_loop(0, chips, split_r, 0)

        def split_l(s, carry):
            block = land_l0[role, pl.ds(2 * s, 2)].astype(F32)
            block = block.reshape(2, 2, rows, count)
            at = pl.ds(pl.multiple_of(s * tile, tile), tile)
            for e in range(2):
                mat_l[e, at, :] = block[:, e].reshape(tile, count).astype(BF16)
            return carry

        lax.fori_loop(0, half, split_l, 0)
        for h in range(2):
            blocks = []
            for e in range(2):
                product = dot(
                    mat_l[e, 0 : half * tile, :], mat_r[e, h * cols : (h + 1) * cols, :], 1, 1
                )
                blocks.append(product.reshape(peers // 2, 1, rows, cols))
            both = jnp.concatenate(blocks, axis=1).reshape(peers // 2, tile, cols)
            tri_out0[role, h] = both.astype(BF16)

    def ready0(chunk):
        role = role_of(chunk)
        waiter(
            land_l0.at[role, pl.ds(0, peers // 2 - 1)], scat_send.at[1, 0], scat_recv0.at[1, role]
        ).wait_recv()
        waiter(
            land_r0.at[role, pl.ds(0, peers // 2)], swap_send.at[0, 0], swap_recv.at[0, role]
        ).wait_recv()
        multiply0(role)

    def give0(chunk, h):
        return_tri(role_of(chunk), h, tri_out0, tri_in0, tri_send.at[0, chunk, h], tri_recv.at[0, h])

    ready0(0)
    give0(0, 0)
    ready0(1)
    give0(1, 0)
    give0(0, 1)
    give0(1, 1)

    def arrived(u, h, tri_in):
        waiter(
            tri_in.at[h, pl.ds(0, peers - 2)], tri_send.at[u, 0, h], tri_recv.at[u, h]
        ).wait_recv()

    for h in range(2):
        arrived(0, h, tri_in0)
        finish(0, h, pair_ref, middle, tri_in0)
        project(1, h, middle)

        def pack1(p, carry):
            at = pl.ds(pl.multiple_of(p * tile, tile), tile)
            src1[h, 0, p] = packed(right_f, at, h * blocks_per_half, blocks_per_half)
            src1[h, 1, p] = packed(left_f, at, h * blocks_per_half, blocks_per_half)
            return carry

        lax.fori_loop(0, peers, pack1, 0, unroll=2)
        for chunk in range(2):
            scatter(
                chunk,
                [
                    (
                        src1.at[h, 0],
                        lambda role, s, h=h: land_r1.at[role, h, s],
                        scat_send.at[2 + 2 * h, chunk],
                        lambda r, h=h: scat_recv1.at[0, h, r],
                    ),
                    (
                        src1.at[h, 1],
                        lambda role, s, h=h: land_l1.at[role, h, s],
                        scat_send.at[3 + 2 * h, chunk],
                        lambda r, h=h: scat_recv1.at[1, h, r],
                    ),
                ],
            )

    gate_values(1)

    def multiply1(role):
        def split(s, carry):
            at = pl.ds(pl.multiple_of(s * tile, tile), tile)
            for land, mat in ((land_l1, mat_l), (land_r1, mat_r)):
                for h in range(2):
                    block = land[role, h, pl.ds(2 * s, 2)].astype(F32)
                    block = block.reshape(2, 2, rows, cols)
                    for e in range(2):
                        mat[e, at, h * cols : (h + 1) * cols] = (
                            block[:, e].reshape(tile, cols).astype(BF16)
                        )
            return carry

        lax.fori_loop(0, half, split, 0)
        depth = half * tile
        for e in range(2):
            for b in range(2):
                a = mat_l[e, 0:depth, b * cols : (b + 1) * cols]
                product = dot(a, mat_r[e, 0:depth, :], 0, 0)
                part[role, b * (peers // 2) : (b + 1) * (peers // 2), e * rows : (e + 1) * rows, :] = (
                    product.reshape(peers // 2, rows, count)
                )

    for chunk in range(2):
        role = role_of(chunk)
        home = owned_set(role)
        for kind, land in ((0, land_r1), (1, land_l1)):
            for h in range(2):
                waiter(
                    land.at[role, h, pl.ds(0, peers // 2 - 1)],
                    scat_send.at[2, 0],
                    scat_recv1.at[kind, h, role],
                ).wait_recv()
        multiply1(role)
        far = base_of(1 - role)

        def round_far(k, carry):
            at = wrap(home + far + k) * 2
            swap_out[role, pl.ds(2 * k, 2)] = part[role, pl.ds(at, 2)].astype(BF16)
            return carry

        lax.fori_loop(0, half, round_far, 0)
        send(
            swap_out.at[role],
            swap_in.at[1 - role],
            swap_send.at[1, chunk],
            swap_recv.at[1, 1 - role],
            chip + SPREAD - 2 * SPREAD * role,
            core,
        )

    def ready1(chunk):
        role = role_of(chunk)
        home = owned_set(role)
        near = base_of(role)
        waiter(swap_in.at[role], swap_send.at[1, 0], swap_recv.at[1, role]).wait_recv()

        def total(k, carry):
            at = wrap(home + near + k) * 2
            both = part[role, pl.ds(at, 2)] + swap_in[role, pl.ds(2 * k, 2)].astype(F32)
            both = both.astype(BF16)
            for h in range(2):
                tri_out1[role, h, pl.ds(2 * k, 2)] = both[:, :, h * cols : (h + 1) * cols]
            return carry

        lax.fori_loop(0, half, total, 0)

    def give1(chunk, h):
        return_tri(role_of(chunk), h, tri_out1, tri_in1, tri_send.at[1, chunk, h], tri_recv.at[1, h])

    ready1(0)
    give1(0, 0)
    ready1(1)
    give1(1, 0)
    give1(0, 1)
    give1(1, 1)

    for h in range(2):
        arrived(1, h, tri_in1)
        finish(1, h, middle, out_ref, tri_in1)

    sent = peers // 2 - 1
    for chunk in range(2):
        for kind in range(2):
            waiter(
                src0.at[kind, pl.ds(0, sent)], scat_send.at[kind, chunk], scat_recv0.at[0, 0]
            ).wait_send()
            for h in range(2):
                waiter(
                    src1.at[h, kind, pl.ds(0, sent)],
                    scat_send.at[2 + 2 * h + kind, chunk],
                    scat_recv0.at[0, 0],
                ).wait_send()
        waiter(
            land_r0.at[0, pl.ds(0, peers // 2)], swap_send.at[0, chunk], swap_recv.at[0, 0]
        ).wait_send()
        waiter(swap_out.at[0], swap_send.at[1, chunk], swap_recv.at[1, 0]).wait_send()
        for h in range(2):
            waiter(
                tri_out0.at[0, h, pl.ds(0, sent)], tri_send.at[0, chunk, h], tri_recv.at[0, h]
            ).wait_send()
            waiter(
                tri_out1.at[0, h, pl.ds(0, sent)], tri_send.at[1, chunk, h], tri_recv.at[1, h]
            ).wait_send()


def per_device(peers, pair_in, valid_tokens, proj_weight, out_weight, norm_gains):
    rows, count, width = pair_in.shape
    cols = count // 2
    tile = 2 * rows
    first_row = lax.axis_index("row") * rows
    valid = valid_tokens.astype(F32)
    mask = lax.dynamic_slice_in_dim(valid, first_row, rows, 0)[:, None] * valid[None, :]
    weight_t = jnp.transpose(proj_weight[:, :, : 4 * width], (0, 2, 1))
    weight_g = proj_weight[:, :, 4 * width :]
    gain_in = norm_gains[:, 0:1, :]
    gain_out = norm_gains[:, 1, :, None]
    vmem = pltpu.VMEM
    dma = pltpu.SemaphoreType.DMA
    near = peers // 2
    block = pl.BlockSpec(memory_space=pltpu.VMEM)
    return pl.pallas_call(
        functools.partial(kernel, peers),
        out_shape=jax.ShapeDtypeStruct((rows, count, width), BF16),
        in_specs=[block] * 7,
        out_specs=block,
        scratch_shapes=[
            vmem((count // LANES, width * rows, LANES), F32),
            vmem((count // LANES, width * rows, LANES), F32),
            vmem((cols // LANES, width * rows, LANES), F32),
            vmem((rows, count, width), BF16),
            vmem((rows, count, width), F32),
            vmem((rows, count, width), BF16),
            vmem((2, peers, tile, count), BF16),
            vmem((2, 2, peers, tile, cols), BF16),
            vmem((2, near, tile, count), BF16),
            vmem((2, peers, tile, count), BF16),
            vmem((2, 2, near, tile, cols), BF16),
            vmem((2, 2, near, tile, cols), BF16),
            vmem((2, count, count), BF16),
            vmem((2, count, count), BF16),
            vmem((2, peers, tile, count), F32),
            vmem((2, 2, near, tile, cols), BF16),
            vmem((2, 2, near, tile, cols), BF16),
            vmem((2, peers, tile, cols), BF16),
            vmem((2, peers, tile, cols), BF16),
            vmem((2, near, tile, count), BF16),
            vmem((2, near, tile, count), BF16),
            dma((6, 2)),
            dma((2, 2)),
            dma((2, 2, 2)),
            dma((2, 2)),
            dma((2, 2)),
            dma((2, 2, 2)),
            dma((2, 2)),
        ],
        compiler_params=pltpu.CompilerParams(
            collective_id=0, has_side_effects=True, vmem_limit_bytes=60 * 1024 * 1024
        ),
    )(pair_in, mask, weight_t, weight_g, out_weight, gain_in, gain_out)


def solution(mesh):
    return jax.shard_map(
        functools.partial(per_device, mesh.shape["row"]),
        mesh=mesh,
        in_specs=(P(("groups", "row"), None, None), P("groups"), P(), P(), P()),
        out_specs=P(("groups", "row"), None, None),
        check_vma=False,
    )
```

```python
import functools

import jax
import jax.numpy as jnp
from jax import lax
from jax.experimental import pallas as pl
from jax.experimental.pallas import tpu as pltpu
from jax.sharding import PartitionSpec as P

MESH = pl.DeviceIdType.MESH
EPSILON = 1e-05
OWNERS = 4
STEP = 3
LANES = 128
BF16 = jnp.bfloat16
F32 = jnp.float32


def dot(a, b, contract_a, contract_b):
    return lax.dot_general(
        a, b, (((contract_a,), (contract_b,)), ((), ())), preferred_element_type=F32
    )


class Plan:
    def __init__(self, peers):
        self.chips = peers // 2
        self.span = (OWNERS - 1) * STEP
        self.outer = (self.chips - self.span - 1) // 2
        self.inner = (STEP - 1) // 2
        edge = self.outer + self.inner + 1
        self.starts = [0] + [edge + STEP * k for k in range(OWNERS - 1)] + [self.chips]
        self.edge = edge
        self.flow = self.chips - edge
        self.deep = 16


def kernel(
    peers,
    pair_ref,
    valid_ref,
    valid_s,
    proj_ref,
    wo_ref,
    gain_ref,
    out_ref,
    wt,
    gain_col,
    left_f,
    right_f,
    tri_f,
    normed,
    gates,
    middle,
    src0,
    src1,
    land_l0,
    land_r0,
    land_l1,
    land_r1,
    mat_l,
    mat_r,
    tri_s,
    part,
    tri_out0,
    tri_out1,
    tri_in0,
    tri_in1,
    flow_out,
    flow_in,
    scat_send,
    scat_recv0,
    scat_recv1,
    relay_send,
    relay_recv,
    flow_send,
    flow_recv,
    tri_send,
    tri_recv,
):
    rows, count, width = pair_ref.shape
    plan = Plan(peers)
    chips, outer, span, starts = plan.chips, plan.outer, plan.span, plan.starts
    cols = count // 2
    blocks_per_half = cols // LANES
    tile = 2 * rows
    me = lax.axis_index("row")
    chip = me // 2
    core = me % 2
    other = 1 - core

    def wrap(a):
        return lax.rem(a + 4 * chips, chips)

    def device(at_chip, at_core):
        return {"row": wrap(at_chip) * 2 + at_core}

    def send(src, dst, ssem, rsem, at_chip, at_core):
        pltpu.make_async_remote_copy(
            src_ref=src,
            dst_ref=dst,
            send_sem=ssem,
            recv_sem=rsem,
            device_id=device(at_chip, at_core),
            device_id_type=MESH,
        ).start()

    def waiter(ref, ssem, rsem):
        return pltpu.make_async_remote_copy(
            src_ref=ref,
            dst_ref=ref,
            send_sem=ssem,
            recv_sem=rsem,
            device_id=device(chip, other),
            device_id_type=MESH,
        )

    def length(role):
        return starts[role + 1] - starts[role]

    def remote(role):
        return 2 * length(role) - 1

    def own_slot(role):
        return outer + STEP * role

    def parity(chunk):
        return lax.rem(chip + chunk, 2)

    def each(chunk, action):
        for role in range(OWNERS):
            pl.when(parity(chunk) == role % 2)(functools.partial(action, role))

    def start_of(role):
        return (plan.edge - STEP + STEP * role) * ((role + OWNERS - 1) // OWNERS)

    def length_of(role):
        end = (2 * role - (OWNERS - 1)) * (2 * role - (OWNERS - 1)) // ((OWNERS - 1) * (OWNERS - 1))
        return STEP + (plan.edge - STEP) * end

    barrier = pltpu.get_barrier_semaphore()
    reach = 2 * outer + 1

    def greet(i, carry):
        at = chip - outer + i
        pl.semaphore_signal(
            barrier, inc=1, device_id=device(at, other), device_id_type=MESH
        )

        @pl.when(i != outer)
        def _():
            pl.semaphore_signal(
                barrier, inc=1, device_id=device(at, core), device_id_type=MESH
            )

        return carry

    lax.fori_loop(0, reach, greet, 0)

    for u in range(2):
        for k in range(4):
            at = slice(k * width, (k + 1) * width)
            wt[u, at, :] = jnp.transpose(proj_ref[u, :, at].astype(F32)).astype(BF16)
        gain_col[u] = jnp.transpose(jnp.broadcast_to(gain_ref[u, 1:2, :], (width, width)))

    def project(u, h, pair):
        there = pl.ds(h * cols, cols)
        valid = valid_ref[:, h * cols : (h + 1) * cols].astype(F32)

        def row(r, carry):
            z = pair[r, there, :].astype(F32)
            mean = jnp.mean(z, axis=1, keepdims=True)
            centered = z - mean
            var = jnp.mean(centered * centered, axis=1, keepdims=True)
            x = (centered * lax.rsqrt(var + EPSILON) * gain_ref[u, 0:1, :]).astype(BF16)
            normed[r, there, :] = x
            m = valid * valid_s[me * rows + r].astype(F32)
            for k, store in ((2, right_f), (0, left_f)):
                gate = dot(wt[u, k * width : (k + 1) * width, :], x, 1, 1)
                value = dot(wt[u, (k + 1) * width : (k + 2) * width, :], x, 1, 1)
                edge = jax.nn.sigmoid(gate) * value * m
                for b in range(blocks_per_half):
                    store[h * blocks_per_half + b, pl.ds(r, width, stride=rows), :] = edge[
                        :, b * LANES : (b + 1) * LANES
                    ]
            return carry

        lax.fori_loop(0, rows, row, 0)

    def gate_values(u):
        def row(r, carry):
            gates[r] = jax.nn.sigmoid(dot(normed[r], proj_ref[u, :, 4 * width :], 1, 0))
            return carry

        lax.fori_loop(0, rows, row, 0)

    def packed(store, at, first, number):
        return jnp.concatenate(
            [store[first + b, at, :] for b in range(number)], axis=1
        ).astype(BF16)

    def finish(u, h, pair, result, tri_in):
        there = pl.ds(h * cols, cols)

        def unpack(p, carry):
            at = pl.ds(pl.multiple_of(p * tile, tile), tile)
            block = tri_in[h, p].astype(F32)
            for b in range(blocks_per_half):
                tri_f[b, at, :] = block[:, b * LANES : (b + 1) * LANES]
            return carry

        lax.fori_loop(0, peers, unpack, 0, unroll=4)

        def row(r, carry):
            t = jnp.concatenate(
                [tri_f[b, pl.ds(r, width, stride=rows), :] for b in range(blocks_per_half)], axis=1
            )
            mean = jnp.mean(t, axis=0, keepdims=True)
            centered = t - mean
            var = jnp.mean(centered * centered, axis=0, keepdims=True)
            scaled = centered * lax.rsqrt(var + EPSILON)
            gain = jnp.concatenate([gain_col[u]] * blocks_per_half, axis=1)
            update = dot((scaled * gain).astype(BF16), wo_ref[u], 0, 0)
            z = pair[r, there, :].astype(F32)
            result[r, there, :] = (z + update * gates[r, there, :]).astype(BF16)
            return carry

        lax.fori_loop(0, rows, row, 0)

    def scatter(chunk, items):
        odd = parity(chunk)

        def step_to(t, role):
            ahead = STEP * role - t
            home = wrap(chip - t)
            slot = t + outer
            for src, dst_of, ssem, rsem in items:
                send(
                    src.at[home * 2 + other],
                    dst_of(role, slot * 2 + core),
                    ssem,
                    rsem(role),
                    chip + ahead,
                    other,
                )

                @pl.when(ahead != 0)
                def _():
                    send(
                        src.at[home * 2 + core],
                        dst_of(role, slot * 2 + core),
                        ssem,
                        rsem(role),
                        chip + ahead,
                        core,
                    )

                @pl.when(ahead == 0)
                def _():
                    dst_of(role, slot * 2 + core)[...] = src[home * 2 + core]

        def outside(k, carry):
            step_to(1 - outer - odd + 2 * k, 0)
            step_to(span + outer - odd - 2 * k, OWNERS - 1)
            return carry

        lax.fori_loop(0, (outer + 1) // 2, outside, 0)

        def inside(k, carry):
            t = 2 - odd + 2 * k
            step_to(t, (t + plan.inner) // STEP)
            return carry

        lax.fori_loop(0, chips // 2 - (outer + 1), inside, 0)

    def return_tri(role, h, tri_out, tri_in, ssem, rsem):
        home = wrap(chip - STEP * role)
        last = starts[role + 1] - 1

        def step(i, carry):
            slot = starts[role] + i if 2 * role < OWNERS else last - i
            at = home - outer + slot
            send(
                tri_out.at[h, slot * 2 + other], tri_in.at[h, home * 2 + core], ssem, rsem, at, other
            )

            @pl.when(slot != own_slot(role))
            def _():
                send(
                    tri_out.at[h, slot * 2 + core],
                    tri_in.at[h, home * 2 + core],
                    ssem,
                    rsem,
                    at,
                    core,
                )

            @pl.when(slot == own_slot(role))
            def _():
                tri_in[h, home * 2 + core] = tri_out[h, slot * 2 + core]

            return carry

        lax.fori_loop(0, length(role), step, 0)

    for h in range(2):
        project(0, h, pair_ref)

    def pack0(p, carry):
        at = pl.ds(pl.multiple_of(p * tile, tile), tile)
        src0[0, p] = packed(right_f, at, 0, 2 * blocks_per_half)
        src0[1, p] = packed(left_f, at, 0, 2 * blocks_per_half)
        return carry

    lax.fori_loop(0, peers, pack0, 0, unroll=2)

    pl.semaphore_wait(barrier, 2 * reach - 1)

    for chunk in range(2):
        scatter(
            chunk,
            [
                (
                    src0.at[0],
                    lambda role, s: land_r0.at[role, s],
                    scat_send.at[0, chunk],
                    lambda r: scat_recv0.at[0, r],
                )
            ],
        )
        scatter(
            chunk,
            [
                (
                    src0.at[1],
                    lambda role, s: land_l0.at[s],
                    scat_send.at[1, chunk],
                    lambda r: scat_recv0.at[1, r],
                )
            ],
        )

    gate_values(0)

    def pieces(role, piece):
        return pl.ds(2 * starts[piece], 2 * length(piece))

    def relay(role, piece, way):
        to = role + way
        if 0 <= to < OWNERS:
            send(
                land_r0.at[role, pieces(role, piece)],
                land_r0.at[to, pieces(role, piece)],
                relay_send.at[role, piece, (way + 1) // 2],
                relay_recv.at[to, piece],
                chip + STEP * way,
                core,
            )

    def relay_own(role):
        ref = land_r0.at[role, pl.ds(0, remote(role))]
        waiter(ref, scat_send.at[0, 0], scat_recv0.at[0, role]).wait_recv()
        relay(role, role, 1)
        relay(role, role, -1)

    def relay_more(gap, role):
        for way in (1, -1):
            piece = role - way * gap
            if 0 <= piece < OWNERS:
                ref = land_r0.at[role, pieces(role, piece)]
                waiter(ref, scat_send.at[0, 0], relay_recv.at[role, piece]).wait_recv()
                relay(role, piece, way)

    for chunk in range(2):
        each(chunk, relay_own)
    for gap in range(1, OWNERS):
        for chunk in range(2):
            each(chunk, functools.partial(relay_more, gap))

    most = plan.edge
    mat_l[...] = jnp.zeros_like(mat_l)
    mat_r[...] = jnp.zeros_like(mat_r)

    def multiply0(role):
        home = wrap(chip - STEP * role)
        start = start_of(role)

        def split_r(s, carry):
            block = land_r0[role, pl.ds(2 * s, 2)].astype(F32)
            block = block.reshape(2, 2, rows, count)
            at = pl.ds(pl.multiple_of(wrap(home - outer + s) * tile, tile), tile)
            for e in range(2):
                mat_r[e, at, :] = block[:, e].reshape(tile, count).astype(BF16)
            return carry

        lax.fori_loop(0, chips, split_r, 0)

        def split_l(s, carry):
            block = land_l0[pl.ds(2 * (start + s), 2)].astype(F32)
            block = block.reshape(2, 2, rows, count)
            at = pl.ds(pl.multiple_of(s * tile, tile), tile)
            for e in range(2):
                mat_l[e, at, :] = block[:, e].reshape(tile, count).astype(BF16)
            return carry

        lax.fori_loop(0, length_of(role), split_l, 0)
        for h in range(2):
            blocks = []
            for e in range(2):
                product = dot(
                    mat_l[e, 0 : most * tile, :], mat_r[e, h * cols : (h + 1) * cols, :], 1, 1
                )
                blocks.append(product.reshape(2 * most, 1, rows, cols))
            both = jnp.concatenate(blocks, axis=1).reshape(2 * most, tile, cols)
            tri_s[h] = both.astype(BF16)

        def keep(s, carry):
            for h in range(2):
                tri_out0[h, pl.ds(2 * (start + s), 2)] = tri_s[h, pl.ds(2 * s, 2)]
            return carry

        lax.fori_loop(0, length_of(role), keep, 0)

    def ready0(chunk):
        def wait_left(role):
            ref = land_l0.at[pl.ds(0, remote(role))]
            waiter(ref, scat_send.at[1, 0], scat_recv0.at[1, role]).wait_recv()

        each(chunk, wait_left)

        def one(i, carry):
            multiply0(parity(chunk) + 2 * i)
            return carry

        lax.fori_loop(0, OWNERS // 2, one, 0)

    def give(u, chunk, h, tri_out, tri_in):
        def one(role):
            return_tri(role, h, tri_out, tri_in, tri_send.at[u, role, h], tri_recv.at[u, h])

        each(chunk, one)

    ready0(0)
    give(0, 0, 0, tri_out0, tri_in0)
    ready0(1)
    give(0, 1, 0, tri_out0, tri_in0)
    give(0, 0, 1, tri_out0, tri_in0)
    give(0, 1, 1, tri_out0, tri_in0)

    def arrived(u, h, tri_in):
        waiter(
            tri_in.at[h, pl.ds(0, peers - OWNERS)], tri_send.at[u, 0, h], tri_recv.at[u, h]
        ).wait_recv()

    for h in range(2):
        arrived(0, h, tri_in0)
        finish(0, h, pair_ref, middle, tri_in0)
        project(1, h, middle)

        def pack1(p, carry):
            at = pl.ds(pl.multiple_of(p * tile, tile), tile)
            src1[h, 0, p] = packed(right_f, at, h * blocks_per_half, blocks_per_half)
            src1[h, 1, p] = packed(left_f, at, h * blocks_per_half, blocks_per_half)
            return carry

        lax.fori_loop(0, peers, pack1, 0, unroll=2)
        for chunk in range(2):
            scatter(
                chunk,
                [
                    (
                        src1.at[h, 0],
                        lambda role, s, h=h: land_r1.at[h, s],
                        scat_send.at[2 + 2 * h, chunk],
                        lambda r, h=h: scat_recv1.at[0, h, r],
                    ),
                    (
                        src1.at[h, 1],
                        lambda role, s, h=h: land_l1.at[h, s],
                        scat_send.at[3 + 2 * h, chunk],
                        lambda r, h=h: scat_recv1.at[1, h, r],
                    ),
                ],
            )

    gate_values(1)

    def multiply1(role):
        start = start_of(role)
        used = length_of(role)

        def split(s, carry):
            at = pl.ds(pl.multiple_of(s * tile, tile), tile)

            @pl.when(s < used)
            def _():
                for land, mat in ((land_l1, mat_l), (land_r1, mat_r)):
                    for h in range(2):
                        block = land[h, pl.ds(2 * (start + s), 2)].astype(F32)
                        block = block.reshape(2, 2, rows, cols)
                        for e in range(2):
                            mat[e, at, h * cols : (h + 1) * cols] = (
                                block[:, e].reshape(tile, cols).astype(BF16)
                            )

            @pl.when(s >= used)
            def _():
                for mat in (mat_l, mat_r):
                    for e in range(2):
                        mat[e, at, :] = jnp.zeros((tile, count), BF16)

            return carry

        lax.fori_loop(0, plan.deep, split, 0)
        depth = plan.deep * tile
        for e in range(2):
            for b in range(2):
                a = mat_l[e, 0:depth, b * cols : (b + 1) * cols]
                product = dot(a, mat_r[e, 0:depth, :], 0, 0)
                part[role, b * (peers // 2) : (b + 1) * (peers // 2), e * rows : (e + 1) * rows, :] = (
                    product.reshape(peers // 2, rows, count)
                )

    flow = plan.flow

    def passing(role, way):
        if way > 0:
            return starts[role + 1], chips, chips - flow, role
        return 0, starts[role], 0, OWNERS - 1 - role

    def flow_on(role, way):
        low, high, first, index = passing(role, way)
        home = wrap(chip - STEP * role)
        side = (way + 1) // 2
        joined = 0 <= role - way < OWNERS
        if joined:
            wait_flow(role, way)

        def step(i, carry):
            slot = low + i
            at = wrap(home - outer + slot) * 2
            there = pl.ds(2 * (slot - first), 2)
            value = part[role, pl.ds(at, 2)]
            if joined:
                value = value + flow_in[side, index - 1, there].astype(F32)
            flow_out[side, index, there] = value.astype(BF16)
            return carry

        lax.fori_loop(0, high - low, step, 0)
        there = pl.ds(2 * (low - first), 2 * (high - low))
        send(
            flow_out.at[side, index, there],
            flow_in.at[side, index, there],
            flow_send.at[side, index],
            flow_recv.at[side, index],
            chip + STEP * way,
            core,
        )

    def wait_flow(role, way):
        low, high, first, index = passing(role - way, way)
        side = (way + 1) // 2
        there = pl.ds(2 * (low - first), 2 * (high - low))
        waiter(
            flow_in.at[side, index, there], flow_send.at[side, index], flow_recv.at[side, index]
        ).wait_recv()

    def begin1(role):
        for kind, land in ((0, land_r1), (1, land_l1)):
            for h in range(2):
                waiter(
                    land.at[h, pl.ds(0, remote(role))], scat_send.at[2, 0], scat_recv1.at[kind, h, role]
                ).wait_recv()

    def flow_stage(stage, role):
        for way in (1, -1):
            source = 0 if way > 0 else OWNERS - 1
            if role == source + way * stage and 0 <= role + way < OWNERS:
                flow_on(role, way)

    for chunk in range(2):
        each(chunk, begin1)

        def one(i, carry):
            multiply1(parity(chunk) + 2 * i)
            return carry

        lax.fori_loop(0, OWNERS // 2, one, 0)
        each(chunk, functools.partial(flow_stage, 0))
    for stage in range(1, OWNERS - 1):
        for chunk in range(2):
            each(chunk, functools.partial(flow_stage, stage))

    def ready1(chunk):
        def one(role):
            home = wrap(chip - STEP * role)
            ends = []
            if role == OWNERS - 1:
                wait_flow(role, 1)
            if role == 0:
                wait_flow(role, -1)
            for way in (1, -1):
                if 0 <= role - way < OWNERS:
                    _, _, first, index = passing(role - way, way)
                    ends.append(((way + 1) // 2, index, first))

            def total(i, carry):
                slot = starts[role] + i
                at = wrap(home - outer + slot) * 2
                value = part[role, pl.ds(at, 2)]
                for side, index, first in ends:
                    value = value + flow_in[side, index, pl.ds(2 * (slot - first), 2)].astype(F32)
                value = value.astype(BF16)
                for h in range(2):
                    tri_out1[h, pl.ds(2 * slot, 2)] = value[:, :, h * cols : (h + 1) * cols]
                return carry

            lax.fori_loop(0, length(role), total, 0)

        each(chunk, one)

    ready1(0)
    give(1, 0, 0, tri_out1, tri_in1)
    ready1(1)
    give(1, 1, 0, tri_out1, tri_in1)
    give(1, 0, 1, tri_out1, tri_in1)
    give(1, 1, 1, tri_out1, tri_in1)

    for h in range(2):
        arrived(1, h, tri_in1)
        finish(1, h, middle, out_ref, tri_in1)

    sent = peers // 2 - OWNERS // 2
    for chunk in range(2):
        for kind in range(2):
            waiter(
                src0.at[kind, pl.ds(0, sent)], scat_send.at[kind, chunk], scat_recv0.at[0, 0]
            ).wait_send()
            for h in range(2):
                waiter(
                    src1.at[h, kind, pl.ds(0, sent)],
                    scat_send.at[2 + 2 * h + kind, chunk],
                    scat_recv0.at[0, 0],
                ).wait_send()
    for role in range(OWNERS):
        for way in (1, -1):
            side = (way + 1) // 2
            if 0 <= role + way < OWNERS:
                low, high, first, index = passing(role, way)
                there = pl.ds(2 * (low - first), 2 * (high - low))
                waiter(
                    flow_out.at[side, index, there], flow_send.at[side, index], flow_recv.at[0, 0]
                ).wait_send()
                for piece in range(OWNERS):
                    if piece == role or (piece < role) == (way > 0):
                        waiter(
                            land_r0.at[role, pieces(role, piece)],
                            relay_send.at[role, piece, side],
                            relay_recv.at[0, 0],
                        ).wait_send()
        for h in range(2):
            for u, tri_out in ((0, tri_out0), (1, tri_out1)):
                waiter(
                    tri_out.at[h, pl.ds(0, remote(role))], tri_send.at[u, role, h], tri_recv.at[u, h]
                ).wait_send()


def per_device(peers, pair_in, valid_tokens, proj_weight, out_weight, norm_gains):
    rows, count, width = pair_in.shape
    cols = count // 2
    tile = 2 * rows
    plan = Plan(peers)
    vmem = pltpu.VMEM
    dma = pltpu.SemaphoreType.DMA
    near = peers // 2
    block = pl.BlockSpec(memory_space=pltpu.VMEM)
    return pl.pallas_call(
        functools.partial(kernel, peers),
        out_shape=jax.ShapeDtypeStruct((rows, count, width), BF16),
        in_specs=[block, block, pl.BlockSpec(memory_space=pltpu.SMEM), block, block, block],
        out_specs=block,
        scratch_shapes=[
            vmem((2, 4 * width, width), BF16),
            vmem((2, width, width), F32),
            vmem((count // LANES, width * rows, LANES), F32),
            vmem((count // LANES, width * rows, LANES), F32),
            vmem((cols // LANES, width * rows, LANES), F32),
            vmem((rows, count, width), BF16),
            vmem((rows, count, width), F32),
            vmem((rows, count, width), BF16),
            vmem((2, peers, tile, count), BF16),
            vmem((2, 2, peers, tile, cols), BF16),
            vmem((peers, tile, count), BF16),
            vmem((OWNERS, peers, tile, count), BF16),
            vmem((2, peers, tile, cols), BF16),
            vmem((2, peers, tile, cols), BF16),
            vmem((2, plan.deep * tile, count), BF16),
            vmem((2, count, count), BF16),
            vmem((2, 2 * plan.edge, tile, cols), BF16),
            vmem((OWNERS, peers, tile, count), F32),
            vmem((2, peers, tile, cols), BF16),
            vmem((2, peers, tile, cols), BF16),
            vmem((2, peers, tile, cols), BF16),
            vmem((2, peers, tile, cols), BF16),
            vmem((2, OWNERS - 1, 2 * plan.flow, tile, count), BF16),
            vmem((2, OWNERS - 1, 2 * plan.flow, tile, count), BF16),
            dma((6, 2)),
            dma((2, OWNERS)),
            dma((2, 2, OWNERS)),
            dma((OWNERS, OWNERS, 2)),
            dma((OWNERS, OWNERS)),
            dma((2, OWNERS - 1)),
            dma((2, OWNERS - 1)),
            dma((2, OWNERS, 2)),
            dma((2, 2)),
        ],
        compiler_params=pltpu.CompilerParams(
            collective_id=0, has_side_effects=True, vmem_limit_bytes=62 * 1024 * 1024
        ),
    )(pair_in, valid_tokens.reshape(1, count), valid_tokens, proj_weight, out_weight, norm_gains)


def solution(mesh):
    return jax.shard_map(
        functools.partial(per_device, mesh.shape["row"]),
        mesh=mesh,
        in_specs=(P(("groups", "row"), None, None), P("groups"), P(), P(), P()),
        out_specs=P(("groups", "row"), None, None),
        check_vma=False,
    )
```

```python
import functools

import jax
import jax.numpy as jnp
from jax import lax
from jax.experimental import pallas as pl
from jax.experimental.pallas import tpu as pltpu
from jax.sharding import PartitionSpec as P

MESH = pl.DeviceIdType.MESH
EPSILON = 1e-05
OWNERS = 4
STEP = 3
LANES = 128
BF16 = jnp.bfloat16
F32 = jnp.float32


def dot(a, b, contract_a, contract_b):
    return lax.dot_general(
        a, b, (((contract_a,), (contract_b,)), ((), ())), preferred_element_type=F32
    )


class Plan:
    def __init__(self, peers):
        self.chips = peers // 2
        self.span = (OWNERS - 1) * STEP
        self.outer = (self.chips - self.span - 1) // 2
        self.inner = (STEP - 1) // 2
        edge = self.outer + self.inner + 1
        self.starts = [0] + [edge + STEP * k for k in range(OWNERS - 1)] + [self.chips]
        self.edge = edge
        self.flow = self.chips - edge
        self.deep = 16


def kernel(
    peers,
    pair_ref,
    valid_ref,
    valid_s,
    proj_ref,
    wo_ref,
    gain_ref,
    out_ref,
    wt,
    gain_col,
    left_f,
    right_f,
    tri_f,
    normed,
    gates,
    middle,
    src0,
    src1,
    land_l0,
    land_r0,
    land1,
    mat_l,
    mat_r,
    tri_s,
    part,
    tri_out0,
    tri_out1,
    tri_in0,
    tri_in1,
    flow_out,
    flow_in,
    scat_send,
    scat_recv0,
    scat_recv1,
    relay_send,
    relay_recv,
    flow_send,
    flow_recv,
    tri_send,
    tri_recv,
):
    rows, count, width = pair_ref.shape
    plan = Plan(peers)
    chips, outer, span, starts = plan.chips, plan.outer, plan.span, plan.starts
    cols = count // 2
    blocks_per_half = cols // LANES
    tile = 2 * rows
    me = lax.axis_index("row")
    chip = me // 2
    core = me % 2
    other = 1 - core

    def wrap(a):
        return lax.rem(a + 4 * chips, chips)

    def device(at_chip, at_core):
        return {"row": wrap(at_chip) * 2 + at_core}

    def send(src, dst, ssem, rsem, at_chip, at_core):
        pltpu.make_async_remote_copy(
            src_ref=src,
            dst_ref=dst,
            send_sem=ssem,
            recv_sem=rsem,
            device_id=device(at_chip, at_core),
            device_id_type=MESH,
        ).start()

    def waiter(ref, ssem, rsem):
        return pltpu.make_async_remote_copy(
            src_ref=ref,
            dst_ref=ref,
            send_sem=ssem,
            recv_sem=rsem,
            device_id=device(chip, other),
            device_id_type=MESH,
        )

    def length(role):
        return starts[role + 1] - starts[role]

    def remote(role):
        return 2 * length(role) - 1

    def start_of(role):
        return (plan.edge - STEP + STEP * role) * ((role + OWNERS - 1) // OWNERS)

    def length_of(role):
        end = (2 * role - (OWNERS - 1)) * (2 * role - (OWNERS - 1)) // ((OWNERS - 1) * (OWNERS - 1))
        return STEP + (plan.edge - STEP) * end

    barrier = pltpu.get_barrier_semaphore()
    reach = 2 * outer + 1

    def greet(i, carry):
        at = chip - outer + i
        pl.semaphore_signal(
            barrier, inc=1, device_id=device(at, other), device_id_type=MESH
        )

        @pl.when(i != outer)
        def _():
            pl.semaphore_signal(
                barrier, inc=1, device_id=device(at, core), device_id_type=MESH
            )

        return carry

    lax.fori_loop(0, reach, greet, 0)

    for u in range(2):
        for k in range(4):
            at = slice(k * width, (k + 1) * width)
            wt[u, at, :] = jnp.transpose(proj_ref[u, :, at].astype(F32)).astype(BF16)
        gain_col[u] = jnp.transpose(jnp.broadcast_to(gain_ref[u, 1:2, :], (width, width)))

    def project(u, h, pair):
        there = pl.ds(h * cols, cols)
        valid = valid_ref[:, h * cols : (h + 1) * cols].astype(F32)

        def row(r, carry):
            z = pair[r, there, :].astype(F32)
            mean = jnp.mean(z, axis=1, keepdims=True)
            centered = z - mean
            var = jnp.mean(centered * centered, axis=1, keepdims=True)
            x = (centered * lax.rsqrt(var + EPSILON) * gain_ref[u, 0:1, :]).astype(BF16)
            normed[r, there, :] = x
            m = valid * valid_s[me * rows + r].astype(F32)
            for k, store in ((2, right_f), (0, left_f)):
                gate = dot(wt[u, k * width : (k + 1) * width, :], x, 1, 1)
                value = dot(wt[u, (k + 1) * width : (k + 2) * width, :], x, 1, 1)
                edge = jax.nn.sigmoid(gate) * value * m
                for b in range(blocks_per_half):
                    store[h * blocks_per_half + b, pl.ds(r, width, stride=rows), :] = edge[
                        :, b * LANES : (b + 1) * LANES
                    ]
            return carry

        lax.fori_loop(0, rows, row, 0)

    def gate_values(u):
        def row(r, carry):
            gates[r] = jax.nn.sigmoid(dot(normed[r], proj_ref[u, :, 4 * width :], 1, 0))
            return carry

        lax.fori_loop(0, rows, row, 0)

    def packed(store, p, e, first, number):
        at = pl.ds(pl.multiple_of(p * tile + e * rows, rows), rows)
        return jnp.concatenate(
            [store[first + b, at, :] for b in range(number)], axis=1
        ).astype(BF16)

    def finish(u, h, pair, result, tri_in):
        there = pl.ds(h * cols, cols)

        def unpack(p, carry):
            for e in range(2):
                at = pl.ds(pl.multiple_of(p * tile + e * rows, rows), rows)
                block = tri_in[h, e, p].astype(F32)
                for b in range(blocks_per_half):
                    tri_f[b, at, :] = block[:, b * LANES : (b + 1) * LANES]
            return carry

        lax.fori_loop(0, peers, unpack, 0, unroll=4)

        def row(r, carry):
            t = jnp.concatenate(
                [tri_f[b, pl.ds(r, width, stride=rows), :] for b in range(blocks_per_half)], axis=1
            )
            mean = jnp.mean(t, axis=0, keepdims=True)
            centered = t - mean
            var = jnp.mean(centered * centered, axis=0, keepdims=True)
            scaled = centered * lax.rsqrt(var + EPSILON)
            gain = jnp.concatenate([gain_col[u]] * blocks_per_half, axis=1)
            update = dot((scaled * gain).astype(BF16), wo_ref[u], 0, 0)
            z = pair[r, there, :].astype(F32)
            result[r, there, :] = (z + update * gates[r, there, :]).astype(BF16)
            return carry

        lax.fori_loop(0, rows, row, 0)

    def scatter(src, dst_of, ssem, rsem):
        def step_to(t, role, owned):
            ahead = STEP * role - t
            home = wrap(chip - t)
            dst = dst_of(role, (t + outer) * 2 + core)
            send(src.at[home * 2 + other], dst, ssem, rsem(role), chip + ahead, other)

            def remote_copy():
                send(src.at[home * 2 + core], dst, ssem, rsem(role), chip + ahead, core)

            if not owned:
                remote_copy()
                return
            pl.when(ahead != 0)(remote_copy)

            @pl.when(ahead == 0)
            def _():
                dst[...] = src[home * 2 + core]

        def outside(k, carry):
            step_to(k - outer, 0, False)
            step_to(span + outer - k, OWNERS - 1, False)
            return carry

        lax.fori_loop(0, outer, outside, 0)

        def inside(t, carry):
            step_to(t, (t + plan.inner) // STEP, True)
            return carry

        lax.fori_loop(0, span + 1, inside, 0)

    def return_tri(u, e, h, tri_out, tri_in):
        ssem = tri_send.at[u, e, h]
        rsem = tri_recv.at[u, e, h]

        def step_to(role, slot, own):
            home = wrap(chip - STEP * role)
            at = home - outer + slot
            dst = tri_in.at[h, e, home * 2 + core]
            send(tri_out.at[h, e, slot * 2 + other], dst, ssem, rsem, at, other)

            @pl.when(jnp.logical_not(own))
            def _():
                send(tri_out.at[h, e, slot * 2 + core], dst, ssem, rsem, at, core)

            @pl.when(own)
            def _():
                dst[...] = tri_out[h, e, slot * 2 + core]

        def ends(i, carry):
            step_to(0, i, i == outer)
            step_to(OWNERS - 1, chips - 1 - i, i == outer)
            return carry

        lax.fori_loop(0, plan.edge, ends, 0)

        def between(i, carry):
            for role in range(1, OWNERS - 1):
                step_to(role, starts[role] + i, i == plan.inner)
            return carry

        lax.fori_loop(0, STEP, between, 0)

    for h in range(2):
        project(0, h, pair_ref)

    def pack0(p, carry):
        for e in range(2):
            src0[0, e, p] = packed(right_f, p, e, 0, 2 * blocks_per_half)
            src0[1, e, p] = packed(left_f, p, e, 0, 2 * blocks_per_half)
        return carry

    lax.fori_loop(0, peers, pack0, 0, unroll=2)

    pl.semaphore_wait(barrier, 2 * reach - 1)

    def scatter_right(e):
        scatter(
            src0.at[0, e],
            lambda role, s: land_r0.at[e, role, s],
            scat_send.at[0, e],
            lambda role: scat_recv0.at[0, e, role],
        )

    def scatter_left(e):
        scatter(
            src0.at[1, e],
            lambda role, s: land_l0.at[e, s],
            scat_send.at[1, e],
            lambda role: scat_recv0.at[1, e, role],
        )

    def pieces(piece):
        return pl.ds(2 * starts[piece], 2 * length(piece))

    def relay(e, role, piece, way):
        to = role + way
        if 0 <= to < OWNERS:
            send(
                land_r0.at[e, role, pieces(piece)],
                land_r0.at[e, to, pieces(piece)],
                relay_send.at[e, role, piece, (way + 1) // 2],
                relay_recv.at[e, to, piece],
                chip + STEP * way,
                core,
            )

    def relay_own(e):
        for role in (0, OWNERS - 1, *range(1, OWNERS - 1)):
            ref = land_r0.at[e, role, pl.ds(0, remote(role))]
            waiter(ref, scat_send.at[0, 0], scat_recv0.at[0, e, role]).wait_recv()
            relay(e, role, role, 1)
            relay(e, role, role, -1)

    def relay_more(e, gap):
        for role in range(OWNERS):
            for way in (1, -1):
                piece = role - way * gap
                if 0 <= piece < OWNERS:
                    ref = land_r0.at[e, role, pieces(piece)]
                    waiter(ref, scat_send.at[0, 0], relay_recv.at[e, role, piece]).wait_recv()
                    relay(e, role, piece, way)

    most = plan.edge
    mat_l[...] = jnp.zeros_like(mat_l)
    mat_r[...] = jnp.zeros_like(mat_r)

    def multiply0(e, role):
        home = wrap(chip - STEP * role)
        start = start_of(role)

        def split_r(s, carry):
            block = land_r0[e, role, pl.ds(2 * s, 2)].astype(F32).reshape(tile, count)
            at = pl.ds(pl.multiple_of(wrap(home - outer + s) * tile, tile), tile)
            mat_r[at, :] = block.astype(BF16)
            return carry

        lax.fori_loop(0, chips, split_r, 0)

        def split_l(s, carry):
            block = land_l0[e, pl.ds(2 * (start + s), 2)].astype(F32).reshape(tile, count)
            at = pl.ds(pl.multiple_of(s * tile, tile), tile)
            mat_l[at, :] = block.astype(BF16)
            return carry

        lax.fori_loop(0, length_of(role), split_l, 0)
        for h in range(2):
            product = dot(mat_l[0 : most * tile, :], mat_r[h * cols : (h + 1) * cols, :], 1, 1)
            tri_s[h] = product.reshape(2 * most, rows, cols).astype(BF16)

        def keep(s, carry):
            for h in range(2):
                tri_out0[h, e, pl.ds(2 * (start + s), 2)] = tri_s[h, pl.ds(2 * s, 2)]
            return carry

        lax.fori_loop(0, length_of(role), keep, 0)

    def multiply_all(multiply, e):
        def one(role, carry):
            multiply(e, role)
            return carry

        lax.fori_loop(0, OWNERS, one, 0)

    def ready0(e):
        for role in range(OWNERS):
            ref = land_l0.at[e, pl.ds(0, remote(role))]
            waiter(ref, scat_send.at[1, 0], scat_recv0.at[1, e, role]).wait_recv()
        multiply_all(multiply0, e)

    scatter_right(0)
    scatter_right(1)
    gate_values(0)
    relay_own(0)
    scatter_left(0)
    relay_own(1)
    relay_more(0, 1)
    scatter_left(1)
    relay_more(1, 1)
    for gap in range(2, OWNERS - 1):
        relay_more(0, gap)
        relay_more(1, gap)
    relay_more(0, OWNERS - 1)
    ready0(0)
    return_tri(0, 0, 0, tri_out0, tri_in0)
    relay_more(1, OWNERS - 1)
    ready0(1)
    return_tri(0, 1, 0, tri_out0, tri_in0)
    return_tri(0, 0, 1, tri_out0, tri_in0)
    return_tri(0, 1, 1, tri_out0, tri_in0)

    def arrived(u, h, tri_in):
        for e in range(2):
            waiter(
                tri_in.at[h, e, pl.ds(0, peers - OWNERS)], tri_send.at[u, 0, h], tri_recv.at[u, e, h]
            ).wait_recv()

    for h in range(2):
        arrived(0, h, tri_in0)
        finish(0, h, pair_ref, middle, tri_in0)
        project(1, h, middle)

        def pack1(p, carry):
            for e in range(2):
                for kind, store in ((0, right_f), (1, left_f)):
                    src1[h, e, p, kind] = packed(store, p, e, h * blocks_per_half, blocks_per_half)
            return carry

        lax.fori_loop(0, peers, pack1, 0, unroll=2)
        for e in range(2):
            scatter(
                src1.at[h, e],
                lambda role, s, h=h, e=e: land1.at[h, e, s],
                scat_send.at[2 + h, e],
                lambda role, h=h, e=e: scat_recv1.at[h, e, role],
            )

    gate_values(1)

    def multiply1(e, role):
        start = start_of(role)
        used = length_of(role)

        def split(s, carry):
            at = pl.ds(pl.multiple_of(s * tile, tile), tile)

            @pl.when(s < used)
            def _():
                for kind, mat in ((1, mat_l), (0, mat_r)):
                    for h in range(2):
                        block = land1[h, e, pl.ds(2 * (start + s), 2), kind].astype(F32)
                        mat[at, h * cols : (h + 1) * cols] = block.reshape(tile, cols).astype(BF16)

            @pl.when(s >= used)
            def _():
                for mat in (mat_l, mat_r):
                    mat[at, :] = jnp.zeros((tile, count), BF16)

            return carry

        lax.fori_loop(0, plan.deep, split, 0)
        depth = plan.deep * tile
        for b in range(2):
            a = mat_l[0:depth, b * cols : (b + 1) * cols]
            product = dot(a, mat_r[0:depth, :], 0, 0)
            part[e, role, b * (peers // 2) : (b + 1) * (peers // 2)] = product.reshape(
                peers // 2, rows, count
            )

    flow = plan.flow

    def passing(role, way):
        if way > 0:
            return starts[role + 1], chips, chips - flow, role
        return 0, starts[role], 0, OWNERS - 1 - role

    def flow_on(e, role, way):
        low, high, first, index = passing(role, way)
        home = wrap(chip - STEP * role)
        side = (way + 1) // 2
        joined = 0 <= role - way < OWNERS
        if joined:
            wait_flow(e, role, way)

        def step(i, carry):
            slot = low + i
            at = wrap(home - outer + slot) * 2
            there = pl.ds(2 * (slot - first), 2)
            value = part[e, role, pl.ds(at, 2)]
            if joined:
                value = value + flow_in[e, side, index - 1, there].astype(F32)
            flow_out[e, side, index, there] = value.astype(BF16)
            return carry

        lax.fori_loop(0, high - low, step, 0)
        there = pl.ds(2 * (low - first), 2 * (high - low))
        send(
            flow_out.at[e, side, index, there],
            flow_in.at[e, side, index, there],
            flow_send.at[e, side, index],
            flow_recv.at[e, side, index],
            chip + STEP * way,
            core,
        )

    def wait_flow(e, role, way):
        low, high, first, index = passing(role - way, way)
        side = (way + 1) // 2
        there = pl.ds(2 * (low - first), 2 * (high - low))
        waiter(
            flow_in.at[e, side, index, there],
            flow_send.at[e, side, index],
            flow_recv.at[e, side, index],
        ).wait_recv()

    def begin1(e):
        for role in range(OWNERS):
            for h in range(2):
                ref = land1.at[h, e, pl.ds(0, remote(role))]
                waiter(ref, scat_send.at[2, 0], scat_recv1.at[h, e, role]).wait_recv()
        multiply_all(multiply1, e)

    def flow_stage(e, stage):
        flow_on(e, stage, 1)
        flow_on(e, OWNERS - 1 - stage, -1)

    for e in range(2):
        begin1(e)
        flow_stage(e, 0)
    for stage in range(1, OWNERS - 1):
        for e in range(2):
            flow_stage(e, stage)

    def ready1(e):
        wait_flow(e, OWNERS - 1, 1)
        wait_flow(e, 0, -1)
        for role in range(OWNERS):
            home = wrap(chip - STEP * role)
            ends = []
            for way in (1, -1):
                if 0 <= role - way < OWNERS:
                    _, _, first, index = passing(role - way, way)
                    ends.append(((way + 1) // 2, index, first))

            def total(i, carry):
                slot = starts[role] + i
                at = wrap(home - outer + slot) * 2
                value = part[e, role, pl.ds(at, 2)]
                for side, index, first in ends:
                    there = pl.ds(2 * (slot - first), 2)
                    value = value + flow_in[e, side, index, there].astype(F32)
                value = value.astype(BF16)
                for h in range(2):
                    tri_out1[h, e, pl.ds(2 * slot, 2)] = value[:, :, h * cols : (h + 1) * cols]
                return carry

            lax.fori_loop(0, length(role), total, 0)

    ready1(0)
    return_tri(1, 0, 0, tri_out1, tri_in1)
    ready1(1)
    return_tri(1, 1, 0, tri_out1, tri_in1)
    return_tri(1, 0, 1, tri_out1, tri_in1)
    return_tri(1, 1, 1, tri_out1, tri_in1)

    for h in range(2):
        arrived(1, h, tri_in1)
        finish(1, h, middle, out_ref, tri_in1)

    sent = peers - OWNERS
    for e in range(2):
        for kind in range(2):
            waiter(
                src0.at[kind, e, pl.ds(0, sent)], scat_send.at[kind, e], scat_recv0.at[0, 0, 0]
            ).wait_send()
        for h in range(2):
            waiter(
                src1.at[h, e, pl.ds(0, sent)], scat_send.at[2 + h, e], scat_recv0.at[0, 0, 0]
            ).wait_send()
            for u, tri_out in ((0, tri_out0), (1, tri_out1)):
                waiter(
                    tri_out.at[h, e, pl.ds(0, sent)], tri_send.at[u, e, h], tri_recv.at[u, e, h]
                ).wait_send()
        for role in range(OWNERS):
            for way in (1, -1):
                side = (way + 1) // 2
                if 0 <= role + way < OWNERS:
                    low, high, first, index = passing(role, way)
                    there = pl.ds(2 * (low - first), 2 * (high - low))
                    waiter(
                        flow_out.at[e, side, index, there],
                        flow_send.at[e, side, index],
                        flow_recv.at[0, 0, 0],
                    ).wait_send()
                    for piece in range(OWNERS):
                        if piece == role or (piece < role) == (way > 0):
                            waiter(
                                land_r0.at[e, role, pieces(piece)],
                                relay_send.at[e, role, piece, side],
                                relay_recv.at[0, 0, 0],
                            ).wait_send()


def per_device(peers, pair_in, valid_tokens, proj_weight, out_weight, norm_gains):
    rows, count, width = pair_in.shape
    cols = count // 2
    tile = 2 * rows
    plan = Plan(peers)
    vmem = pltpu.VMEM
    dma = pltpu.SemaphoreType.DMA
    block = pl.BlockSpec(memory_space=pltpu.VMEM)
    return pl.pallas_call(
        functools.partial(kernel, peers),
        out_shape=jax.ShapeDtypeStruct((rows, count, width), BF16),
        in_specs=[block, block, pl.BlockSpec(memory_space=pltpu.SMEM), block, block, block],
        out_specs=block,
        scratch_shapes=[
            vmem((2, 4 * width, width), BF16),
            vmem((2, width, width), F32),
            vmem((count // LANES, width * rows, LANES), F32),
            vmem((count // LANES, width * rows, LANES), F32),
            vmem((cols // LANES, width * rows, LANES), F32),
            vmem((rows, count, width), BF16),
            vmem((rows, count, width), F32),
            vmem((rows, count, width), BF16),
            vmem((2, 2, peers, rows, count), BF16),
            vmem((2, 2, peers, 2, rows, cols), BF16),
            vmem((2, peers, rows, count), BF16),
            vmem((2, OWNERS, peers, rows, count), BF16),
            vmem((2, 2, peers, 2, rows, cols), BF16),
            vmem((plan.deep * tile, count), BF16),
            vmem((count, count), BF16),
            vmem((2, 2 * plan.edge, rows, cols), BF16),
            vmem((2, OWNERS, peers, rows, count), F32),
            vmem((2, 2, peers, rows, cols), BF16),
            vmem((2, 2, peers, rows, cols), BF16),
            vmem((2, 2, peers, rows, cols), BF16),
            vmem((2, 2, peers, rows, cols), BF16),
            vmem((2, 2, OWNERS - 1, 2 * plan.flow, rows, count), BF16),
            vmem((2, 2, OWNERS - 1, 2 * plan.flow, rows, count), BF16),
            dma((4, 2)),
            dma((2, 2, OWNERS)),
            dma((2, 2, OWNERS)),
            dma((2, OWNERS, OWNERS, 2)),
            dma((2, OWNERS, OWNERS)),
            dma((2, 2, OWNERS - 1)),
            dma((2, 2, OWNERS - 1)),
            dma((2, 2, 2)),
            dma((2, 2, 2)),
        ],
        compiler_params=pltpu.CompilerParams(
            collective_id=0, has_side_effects=True, vmem_limit_bytes=62 * 1024 * 1024
        ),
    )(pair_in, valid_tokens.reshape(1, count), valid_tokens, proj_weight, out_weight, norm_gains)


def solution(mesh):
    return jax.shard_map(
        functools.partial(per_device, mesh.shape["row"]),
        mesh=mesh,
        in_specs=(P(("groups", "row"), None, None), P("groups"), P(), P(), P()),
        out_specs=P(("groups", "row"), None, None),
        check_vma=False,
    )
```

```python
import functools

import jax
import jax.numpy as jnp
from jax import lax
from jax.experimental import pallas as pl
from jax.experimental.pallas import tpu as pltpu
from jax.sharding import PartitionSpec as P

MESH = pl.DeviceIdType.MESH
EPSILON = 1e-05
COLUMNS = 4
PARTS = 4
LANES = 128
BF16 = jnp.bfloat16
F32 = jnp.float32


def dot(a, b, contract_a, contract_b):
    return lax.dot_general(
        a, b, (((contract_a,), (contract_b,)), ((), ())), preferred_element_type=F32
    )


def kernel(
    peers,
    across,
    pair_ref,
    valid_ref,
    proj_ref,
    wo_ref,
    gain_ref,
    out_ref,
    wt,
    gain_col,
    left_f,
    right_f,
    tri_f,
    normed,
    gates,
    valid_own,
    valid_got,
    start_z,
    middle,
    final_z,
    home_z,
    relay_in,
    relay_out,
    src,
    land,
    mat_l,
    mat_r,
    tri_out,
    tri_in,
    valid_send,
    valid_recv,
    in_send,
    in_recv,
    in_relay_send,
    in_relay_recv,
    out_send,
    out_recv,
    out_relay_send,
    out_relay_recv,
    scat_send,
    scat_recv,
    tri_send,
    tri_recv,
):
    rows, count, width = pair_ref.shape
    chips = peers // 2
    length = chips // COLUMNS
    side = length // 2
    outer = (chips - length) // 2
    cols = count // 2
    part_cols = count // PARTS
    blocks_per_half = cols // LANES
    tile = 2 * rows
    me = lax.axis_index("row")
    chip = me // 2
    core = me % 2
    other = 1 - core
    group = lax.axis_index("groups")
    down = (group // across) % 2
    right = (group % across) % 2
    column = 2 * down + right
    block = chip // length
    offset = chip % length

    def device(at_column, at_chip, at_core):
        at_group = group + (at_column // 2 - down) * across + (at_column % 2 - right)
        return {"groups": at_group, "row": at_chip * 2 + at_core}

    def copier(from_ref, to_ref, ssem, rsem, at):
        return pltpu.make_async_remote_copy(
            src_ref=from_ref,
            dst_ref=to_ref,
            send_sem=ssem,
            recv_sem=rsem,
            device_id=at,
            device_id_type=MESH,
        )

    def send(from_ref, to_ref, ssem, rsem, at):
        copier(from_ref, to_ref, ssem, rsem, at).start()

    def waiter(ref, ssem, rsem):
        return copier(ref, ref, ssem, rsem, device(column, chip, other))

    def mirror(half, value):
        return value + half * (length - 1 - 2 * value)

    def placed(at_chip, of_group):
        t = (at_chip - length * of_group + outer + chips) % chips - outer
        half = (t + outer) // (2 * length)
        a = mirror(half, t) + outer
        at_column = a % COLUMNS
        w = (at_column + 1 + a // COLUMNS) % COLUMNS
        return at_column, length * of_group + mirror(half, w)

    def origin(at_column, at_offset):
        half = at_offset // side
        w = mirror(half, at_offset)
        k = (w - at_column - 1 + 2 * COLUMNS) % COLUMNS
        t = mirror(half, COLUMNS * k + at_column - outer)
        return (length * block + t + chips) % chips

    to_column, to_chip = placed(chip, column)
    from_chip = origin(column, offset)
    mine = from_chip * 2 + core
    owner = (offset * COLUMNS + column) * 2 + core
    stays = jnp.logical_and(to_column == column, to_chip == chip)
    moves = jnp.logical_not(stays)

    barrier = pltpu.get_barrier_semaphore()

    def greet_block(k, carry):
        at_chip = length * block + (offset + k) % length
        for i in range(COLUMNS):
            at_column = (column + i) % COLUMNS
            at = device(at_column, at_chip, other)
            pl.semaphore_signal(barrier, inc=1, device_id=at, device_id_type=MESH)
            at = device(at_column, at_chip, core)
            if i == 0:

                @pl.when(k != 0)
                def _():
                    pl.semaphore_signal(barrier, inc=1, device_id=at, device_id_type=MESH)
            else:
                pl.semaphore_signal(barrier, inc=1, device_id=at, device_id_type=MESH)
        return carry

    lax.fori_loop(0, length, greet_block, 0)

    def greet_column(k, carry):
        at = device(column, (length * (block + 1) + k) % chips, core)
        pl.semaphore_signal(barrier, inc=1, device_id=at, device_id_type=MESH)
        return carry

    lax.fori_loop(0, chips - length, greet_column, 0)

    valid_own[...] = jnp.broadcast_to(valid_ref[...].astype(F32), valid_own.shape)

    for u in range(2):
        for k in range(4):
            at = slice(k * width, (k + 1) * width)
            wt[u, at, :] = jnp.transpose(proj_ref[u, :, at].astype(F32)).astype(BF16)
        gain_col[u] = jnp.transpose(jnp.broadcast_to(gain_ref[u, 1:2, :], (width, width)))

    pl.semaphore_wait(barrier, 2 * COLUMNS * length - 1 + chips - length)

    def part(ref, f):
        return ref.at[:, pl.ds(f * part_cols, part_cols), :]

    two_steps = jnp.logical_and(to_column != column, to_chip != chip)
    one_step = jnp.logical_and(moves, jnp.logical_not(two_steps))

    @pl.when(block == column)
    def _():
        for i in range(1, COLUMNS):
            at = device((column + i) % COLUMNS, chip, core)
            send(valid_own, valid_got, valid_send.at[i - 1], valid_recv, at)
        valid_got[...] = valid_own[...]

    for f in range(PARTS):

        @pl.when(two_steps)
        def _():
            at = device(to_column, chip, core)
            dst = relay_in.at[column, :, pl.ds(f * part_cols, part_cols), :]
            send(part(pair_ref, f), dst, in_send.at[f], in_relay_recv.at[column, f], at)

        @pl.when(one_step)
        def _():
            at = device(to_column, to_chip, core)
            send(part(pair_ref, f), part(start_z, f), in_send.at[f], in_recv.at[f], at)

    @pl.when(stays)
    def _():
        start_z[...] = pair_ref[...]

    def each_relay(action):
        for b in range(COLUMNS):
            at_column, at_chip = placed(chip, b)
            here = jnp.logical_and(at_column == column, at_chip != chip)
            pl.when(jnp.logical_and(here, column != b))(functools.partial(action, b, at_chip))

    def relay_part(ref, b, f):
        return ref.at[b, :, pl.ds(f * part_cols, part_cols), :]

    for f in range(PARTS):

        def pass_in(b, at_chip):
            held = relay_part(relay_in, b, f)
            waiter(held, in_send.at[0], in_relay_recv.at[b, f]).wait_recv()
            at = device(column, at_chip, core)
            send(held, part(start_z, f), in_relay_send.at[b, f], in_recv.at[f], at)

        each_relay(pass_in)

    @pl.when(block != column)
    def _():
        waiter(valid_got, valid_send.at[0], valid_recv).wait_recv()

    def project(u, h, pair):
        there = pl.ds(h * cols, cols)
        valid = valid_got[0:1, h * cols : (h + 1) * cols]
        token = lax.broadcasted_iota(jnp.int32, (1, count), 1)

        def row(r, carry):
            z = pair[r, there, :].astype(F32)
            mean = jnp.mean(z, axis=1, keepdims=True)
            centered = z - mean
            var = jnp.mean(centered * centered, axis=1, keepdims=True)
            x = (centered * lax.rsqrt(var + EPSILON) * gain_ref[u, 0:1, :]).astype(BF16)
            normed[r, there, :] = x
            own = jnp.where(token == mine * rows + r, valid_got[0:1, :], 0.0)
            m = valid * jnp.sum(own, axis=1, keepdims=True)
            for k, store in ((2, right_f), (0, left_f)):
                gate = dot(wt[u, k * width : (k + 1) * width, :], x, 1, 1)
                value = dot(wt[u, (k + 1) * width : (k + 2) * width, :], x, 1, 1)
                edge = jax.nn.sigmoid(gate) * value * m
                for b in range(blocks_per_half):
                    store[h * blocks_per_half + b, pl.ds(r, width, stride=rows), :] = edge[
                        :, b * LANES : (b + 1) * LANES
                    ]
            return carry

        lax.fori_loop(0, rows, row, 0)

    def gate_values(u):
        def row(r, carry):
            gates[r] = jax.nn.sigmoid(dot(normed[r], proj_ref[u, :, 4 * width :], 1, 0))
            return carry

        lax.fori_loop(0, rows, row, 0)

    def packed(store, p, e, first, number):
        at = pl.ds(pl.multiple_of(p * tile + e * rows, rows), rows)
        return jnp.concatenate(
            [store[first + b, at, :] for b in range(number)], axis=1
        ).astype(BF16)

    def finish(u, h, pair, result):
        there = pl.ds(h * cols, cols)

        def unpack(p, carry):
            for e in range(2):
                at = pl.ds(pl.multiple_of(p * tile + e * rows, rows), rows)
                block = tri_in[u, h, e, p].astype(F32)
                for b in range(blocks_per_half):
                    tri_f[b, at, :] = block[:, b * LANES : (b + 1) * LANES]
            return carry

        lax.fori_loop(0, peers, unpack, 0, unroll=4)

        def row(r, carry):
            t = jnp.concatenate(
                [tri_f[b, pl.ds(r, width, stride=rows), :] for b in range(blocks_per_half)], axis=1
            )
            mean = jnp.mean(t, axis=0, keepdims=True)
            centered = t - mean
            var = jnp.mean(centered * centered, axis=0, keepdims=True)
            scaled = centered * lax.rsqrt(var + EPSILON)
            gain = jnp.concatenate([gain_col[u]] * blocks_per_half, axis=1)
            update = dot((scaled * gain).astype(BF16), wo_ref[u], 0, 0)
            z = pair[r, there, :].astype(F32)
            result[r, there, :] = (z + update * gates[r, there, :]).astype(BF16)
            return carry

        lax.fori_loop(0, rows, row, 0)

    def each_member(action):
        def step(k, carry):
            at_offset = (offset + side + k) % length
            for cc in (other, core):
                for i in range(COLUMNS):
                    at_column = (column + i) % COLUMNS
                    may_be_self = i == 0 and cc is core
                    action(at_column, at_offset, cc, k == side if may_be_self else None)
            return carry

        lax.fori_loop(0, length, step, 0)

    def send_or_keep(from_ref, to_ref, ssem, rsem, at, own):
        if own is None:
            send(from_ref, to_ref, ssem, rsem, at)
            return

        @pl.when(jnp.logical_not(own))
        def _():
            send(from_ref, to_ref, ssem, rsem, at)

        @pl.when(own)
        def _():
            to_ref[...] = from_ref[...]

    def scatter(u, h, e):
        def one(at_column, at_offset, at_core, own):
            at_owner = (at_offset * COLUMNS + at_column) * 2 + at_core
            send_or_keep(
                src.at[u, h, e, at_owner],
                land.at[u, h, e, mine],
                scat_send.at[u, h, e],
                scat_recv.at[u, h, e],
                device(at_column, length * block + at_offset, at_core),
                own,
            )

        each_member(one)

    def return_tri(u, e, h):
        def one(at_column, at_offset, at_core, own):
            at_rows = origin(at_column, at_offset) * 2 + at_core
            send_or_keep(
                tri_out.at[u, h, e, at_rows],
                tri_in.at[u, h, e, owner],
                tri_send.at[u, h, e],
                tri_recv.at[u, h, e],
                device(at_column, length * block + at_offset, at_core),
                own,
            )

        each_member(one)

    def edges(u, h, z):
        project(u, h, z)

        def pack(p, carry):
            for e in range(2):
                for kind, store in ((0, right_f), (1, left_f)):
                    src[u, h, e, p, kind] = packed(store, p, e, h * blocks_per_half, blocks_per_half)
            return carry

        lax.fori_loop(0, peers, pack, 0, unroll=2)
        for e in range(2):
            scatter(u, h, e)

    def multiply(u, e):
        for h in range(2):
            ref = land.at[u, h, e, pl.ds(0, peers - 1)]
            waiter(ref, scat_send.at[0, 0, 0], scat_recv.at[u, h, e]).wait_recv()

        def split(s, carry):
            at = pl.ds(pl.multiple_of(s * tile, tile), tile)
            for kind, mat in ((1, mat_l), (0, mat_r)):
                for h in range(2):
                    edge = land[u, h, e, pl.ds(2 * s, 2), kind].astype(F32)
                    mat[at, h * cols : (h + 1) * cols] = edge.reshape(tile, cols).astype(BF16)
            return carry

        lax.fori_loop(0, chips, split, 0)
        some = peers // 2
        for b in range(2):
            for h in range(2):
                first, second = slice(b * cols, (b + 1) * cols), slice(h * cols, (h + 1) * cols)
                if u == 0:
                    product = dot(mat_l[first, :], mat_r[second, :], 1, 1)
                else:
                    product = dot(mat_l[:, first], mat_r[:, second], 0, 0)
                tri_out[u, h, e, b * some : (b + 1) * some] = product.reshape(
                    some, rows, cols
                ).astype(BF16)

    def triangle(u):
        multiply(u, 0)
        return_tri(u, 0, 0)
        multiply(u, 1)
        return_tri(u, 1, 0)
        return_tri(u, 0, 1)
        return_tri(u, 1, 1)

    def arrived(u, h):
        for e in range(2):
            ref = tri_in.at[u, h, e, pl.ds(0, peers - 1)]
            waiter(ref, tri_send.at[0, 0, 0], tri_recv.at[u, h, e]).wait_recv()

    per_half = PARTS // 2

    for h in range(2):
        for f in range(h * per_half, (h + 1) * per_half):

            @pl.when(moves)
            def _():
                waiter(part(start_z, f), in_send.at[0], in_recv.at[f]).wait_recv()

        edges(0, h, start_z)
    gate_values(0)
    triangle(0)

    for h in range(2):
        arrived(0, h)
        finish(0, h, start_z, middle)
        edges(1, h, middle)
    gate_values(1)
    triangle(1)

    far = from_chip != chip
    away = jnp.logical_and(far, column != block)
    near = jnp.logical_and(moves, jnp.logical_not(away))
    for h in range(2):
        arrived(1, h)
        finish(1, h, middle, final_z)
        for f in range(h * per_half, (h + 1) * per_half):

            @pl.when(away)
            def _():
                at = device(column, from_chip, core)
                held = relay_part(relay_out, block, f)
                send(part(final_z, f), held, out_send.at[f], out_relay_recv.at[block, f], at)

            @pl.when(near)
            def _():
                at = device(block, from_chip, core)
                send(part(final_z, f), part(home_z, f), out_send.at[f], out_recv.at[f], at)

    for f in range(PARTS):

        def pass_out(b, at_chip):
            held = relay_part(relay_out, b, f)
            waiter(held, out_send.at[0], out_relay_recv.at[b, f]).wait_recv()
            at = device(b, chip, core)
            send(held, part(home_z, f), out_relay_send.at[b, f], out_recv.at[f], at)

        each_relay(pass_out)

    for f in range(PARTS):
        there = pl.ds(f * part_cols, part_cols)

        @pl.when(moves)
        def _():
            waiter(part(home_z, f), out_send.at[0], out_recv.at[f]).wait_recv()
            out_ref[:, there, :] = home_z[:, there, :]

        @pl.when(stays)
        def _():
            out_ref[:, there, :] = final_z[:, there, :]

    @pl.when(block == column)
    def _():
        for i in range(1, COLUMNS):
            waiter(valid_own, valid_send.at[i - 1], valid_recv).wait_send()

    @pl.when(moves)
    def _():
        for f in range(PARTS):
            waiter(part(pair_ref, f), in_send.at[f], in_recv.at[f]).wait_send()
            waiter(part(final_z, f), out_send.at[f], out_recv.at[f]).wait_send()

    def left_relay(b, at_chip):
        for f in range(PARTS):
            waiter(relay_part(relay_in, b, f), in_relay_send.at[b, f], in_recv.at[f]).wait_send()
            waiter(relay_part(relay_out, b, f), out_relay_send.at[b, f], out_recv.at[f]).wait_send()

    each_relay(left_relay)
    for u in range(2):
        for h in range(2):
            for e in range(2):
                waiter(
                    src.at[u, h, e, pl.ds(0, peers - 1)], scat_send.at[u, h, e], scat_recv.at[u, h, e]
                ).wait_send()
                waiter(
                    tri_out.at[u, h, e, pl.ds(0, peers - 1)], tri_send.at[u, h, e], tri_recv.at[u, h, e]
                ).wait_send()


def per_device(peers, across, pair_in, valid_tokens, proj_weight, out_weight, norm_gains):
    rows, count, width = pair_in.shape
    cols = count // 2
    vmem = pltpu.VMEM
    dma = pltpu.SemaphoreType.DMA
    pair = vmem((rows, count, width), BF16)
    relayed = vmem((COLUMNS, rows, count, width), BF16)
    edge_tiles = vmem((2, 2, 2, peers, 2, rows, cols), BF16)
    tri_tiles = vmem((2, 2, 2, peers, rows, cols), BF16)
    whole = pl.BlockSpec(memory_space=pltpu.VMEM)
    return pl.pallas_call(
        functools.partial(kernel, peers, across),
        out_shape=jax.ShapeDtypeStruct((rows, count, width), BF16),
        in_specs=[whole] * 5,
        out_specs=whole,
        scratch_shapes=[
            vmem((2, 4 * width, width), BF16),
            vmem((2, width, width), F32),
            vmem((count // LANES, width * rows, LANES), F32),
            vmem((count // LANES, width * rows, LANES), F32),
            vmem((cols // LANES, width * rows, LANES), F32),
            pair,
            vmem((rows, count, width), F32),
            vmem((8, count), F32),
            vmem((8, count), F32),
            pair,
            pair,
            pair,
            pair,
            relayed,
            relayed,
            edge_tiles,
            edge_tiles,
            vmem((count, count), BF16),
            vmem((count, count), BF16),
            tri_tiles,
            tri_tiles,
            dma((COLUMNS - 1,)),
            dma,
            dma((PARTS,)),
            dma((PARTS,)),
            dma((COLUMNS, PARTS)),
            dma((COLUMNS, PARTS)),
            dma((PARTS,)),
            dma((PARTS,)),
            dma((COLUMNS, PARTS)),
            dma((COLUMNS, PARTS)),
            dma((2, 2, 2)),
            dma((2, 2, 2)),
            dma((2, 2, 2)),
            dma((2, 2, 2)),
        ],
        compiler_params=pltpu.CompilerParams(
            collective_id=0, has_side_effects=True, vmem_limit_bytes=60 * 1024 * 1024
        ),
    )(pair_in, valid_tokens.reshape(1, count), proj_weight, out_weight, norm_gains)


def solution(mesh):
    across = len({d.coords[0] for d in mesh.devices[:, 0]})
    return jax.shard_map(
        functools.partial(per_device, mesh.shape["row"], across),
        mesh=mesh,
        in_specs=(P(("groups", "row"), None, None), P("groups"), P(), P(), P()),
        out_specs=P(("groups", "row"), None, None),
        check_vma=False,
    )
```

```python
import functools

import jax
import jax.numpy as jnp
from jax import lax
from jax.experimental import pallas as pl
from jax.experimental.pallas import tpu as pltpu
from jax.sharding import PartitionSpec as P

MESH = pl.DeviceIdType.MESH
EPSILON = 1e-05
COLUMNS = 4
LANES = 128
BF16 = jnp.bfloat16
F32 = jnp.float32


def dot(a, b, contract_a, contract_b):
    return lax.dot_general(
        a, b, (((contract_a,), (contract_b,)), ((), ())), preferred_element_type=F32
    )


def kernel(
    peers,
    across,
    pair_ref,
    valid_ref,
    proj_ref,
    wo_ref,
    gain_ref,
    out_ref,
    wt,
    gain_col,
    left_f,
    right_f,
    tri_f,
    normed,
    gates,
    valid_own,
    valid_got,
    start_z,
    middle,
    final_z,
    home_z,
    relay_in,
    relay_out,
    src,
    land,
    mat_l,
    mat_r,
    tri_out,
    tri_in,
    valid_send,
    valid_recv,
    in_send,
    in_recv,
    in_relay_send,
    in_relay_recv,
    out_send,
    out_recv,
    out_relay_send,
    out_relay_recv,
    scat_send,
    scat_recv,
    tri_send,
    tri_recv,
    calm,
):
    rows, count, width = pair_ref.shape
    chips = peers // 2
    length = chips // COLUMNS
    side = length // 2
    outer = (chips - length) // 2
    cols = count // 2
    part_cols = LANES
    parts = count // LANES
    blocks_per_half = cols // LANES
    tile = 2 * rows
    me = lax.axis_index("row")
    chip = me // 2
    core = me % 2
    other = 1 - core
    group = lax.axis_index("groups")
    down = (group // across) % 2
    right = (group % across) % 2
    column = 2 * down + right
    block = chip // length
    offset = chip % length

    def device(at_column, at_chip, at_core):
        at_group = group + (at_column // 2 - down) * across + (at_column % 2 - right)
        return {"groups": at_group, "row": at_chip * 2 + at_core}

    def copier(from_ref, to_ref, ssem, rsem, at):
        return pltpu.make_async_remote_copy(
            src_ref=from_ref,
            dst_ref=to_ref,
            send_sem=ssem,
            recv_sem=rsem,
            device_id=at,
            device_id_type=MESH,
        )

    def send(from_ref, to_ref, ssem, rsem, at):
        copier(from_ref, to_ref, ssem, rsem, at).start()

    def waiter(ref, ssem, rsem):
        return copier(ref, ref, ssem, rsem, device(column, chip, other))

    def mirror(half, value):
        return value + half * (length - 1 - 2 * value)

    def placed(at_chip, of_group):
        t = (at_chip - length * of_group + outer + chips) % chips - outer
        half = (t + outer) // (2 * length)
        a = mirror(half, t) + outer
        turn = a % COLUMNS
        w = (turn + 1 + a // COLUMNS) % COLUMNS
        return (turn + of_group) % COLUMNS, length * of_group + mirror(half, w)

    def origin(at_column, at_offset):
        half = at_offset // side
        w = mirror(half, at_offset)
        turn = (at_column - block + COLUMNS) % COLUMNS
        k = (w - turn - 1 + 2 * COLUMNS) % COLUMNS
        t = mirror(half, COLUMNS * k + turn - outer)
        return (length * block + t + chips) % chips

    to_column, to_chip = placed(chip, column)
    from_chip = origin(column, offset)
    mine = from_chip * 2 + core
    owner = (offset * COLUMNS + column) * 2 + core
    stays = jnp.logical_and(to_column == column, to_chip == chip)
    moves = jnp.logical_not(stays)

    barrier = pltpu.get_barrier_semaphore()

    def greet_block(k, carry):
        at_chip = length * block + (offset + k) % length
        for i in range(COLUMNS):
            at_column = (column + i) % COLUMNS
            at = device(at_column, at_chip, other)
            pl.semaphore_signal(barrier, inc=1, device_id=at, device_id_type=MESH)
            at = device(at_column, at_chip, core)
            if i == 0:

                @pl.when(k != 0)
                def _():
                    pl.semaphore_signal(barrier, inc=1, device_id=at, device_id_type=MESH)
            else:
                pl.semaphore_signal(barrier, inc=1, device_id=at, device_id_type=MESH)
        return carry

    lax.fori_loop(0, length, greet_block, 0)

    def greet_column(k, carry):
        at = device(column, (length * (block + 1) + k) % chips, core)
        pl.semaphore_signal(barrier, inc=1, device_id=at, device_id_type=MESH)
        return carry

    lax.fori_loop(0, chips - length, greet_column, 0)

    valid_own[...] = jnp.broadcast_to(valid_ref[...].astype(F32), valid_own.shape)

    for u in range(2):
        for k in range(4):
            at = slice(k * width, (k + 1) * width)
            wt[u, at, :] = jnp.transpose(proj_ref[u, :, at].astype(F32)).astype(BF16)
        gain_col[u] = jnp.transpose(jnp.broadcast_to(gain_ref[u, 1:2, :], (width, width)))

    pl.semaphore_wait(barrier, 2 * COLUMNS * length - 1 + chips - length)

    def part(ref, f):
        return ref.at[:, pl.ds(f * part_cols, part_cols), :]

    two_steps = jnp.logical_and(to_column != column, to_chip != chip)
    one_step = jnp.logical_and(moves, jnp.logical_not(two_steps))

    @pl.when(block == column)
    def _():
        for i in range(1, COLUMNS):
            at = device((column + i) % COLUMNS, chip, core)
            send(valid_own, valid_got, valid_send.at[i - 1], valid_recv, at)
        valid_got[...] = valid_own[...]

    for f in range(parts):

        @pl.when(two_steps)
        def _():
            at = device(to_column, chip, core)
            dst = relay_in.at[column, :, pl.ds(f * part_cols, part_cols), :]
            send(part(pair_ref, f), dst, in_send.at[f], in_relay_recv.at[column, f], at)

        @pl.when(one_step)
        def _():
            at = device(to_column, to_chip, core)
            send(part(pair_ref, f), part(start_z, f), in_send.at[f], in_recv.at[f], at)

    @pl.when(stays)
    def _():
        start_z[...] = pair_ref[...]

    def each_relay(action):
        for b in range(COLUMNS):
            at_column, at_chip = placed(chip, b)
            here = jnp.logical_and(at_column == column, at_chip != chip)
            pl.when(jnp.logical_and(here, column != b))(functools.partial(action, b, at_chip))

    def relay_part(ref, b, f):
        return ref.at[b, :, pl.ds(f * part_cols, part_cols), :]

    for f in range(parts):

        def pass_in(b, at_chip):
            held = relay_part(relay_in, b, f)
            waiter(held, in_send.at[0], in_relay_recv.at[b, f]).wait_recv()
            at = device(column, at_chip, core)
            send(held, part(start_z, f), in_relay_send.at[b, f], in_recv.at[f], at)

        each_relay(pass_in)

    @pl.when(block != column)
    def _():
        waiter(valid_got, valid_send.at[0], valid_recv).wait_recv()

    def project(u, first, number, pair):
        there = pl.ds(first * LANES, number * LANES)
        valid = valid_got[0:1, first * LANES : (first + number) * LANES]
        token = lax.broadcasted_iota(jnp.int32, (1, count), 1)

        def row(r, carry):
            z = pair[r, there, :].astype(F32)
            mean = jnp.mean(z, axis=1, keepdims=True)
            centered = z - mean
            var = jnp.mean(centered * centered, axis=1, keepdims=True)
            x = (centered * lax.rsqrt(var + EPSILON) * gain_ref[u, 0:1, :]).astype(BF16)
            normed[r, there, :] = x
            own = jnp.where(token == mine * rows + r, valid_got[0:1, :], 0.0)
            m = valid * jnp.sum(own, axis=1, keepdims=True)
            for k, store in ((2, right_f), (0, left_f)):
                gate = dot(wt[u, k * width : (k + 1) * width, :], x, 1, 1)
                value = dot(wt[u, (k + 1) * width : (k + 2) * width, :], x, 1, 1)
                edge = jax.nn.sigmoid(gate) * value * m
                for b in range(number):
                    store[first + b, pl.ds(r, width, stride=rows), :] = edge[
                        :, b * LANES : (b + 1) * LANES
                    ]
            return carry

        lax.fori_loop(0, rows, row, 0)

    def gate_values(u):
        def row(r, carry):
            gates[r] = jax.nn.sigmoid(dot(normed[r], proj_ref[u, :, 4 * width :], 1, 0))
            return carry

        lax.fori_loop(0, rows, row, 0)

    def finish(u, h, pair, result):
        there = pl.ds(h * cols, cols)

        def unpack(p, carry):
            for e in range(2):
                at = pl.ds(pl.multiple_of(p * tile + e * rows, rows), rows)
                block = tri_in[u, h, e, p].astype(F32)
                for b in range(blocks_per_half):
                    tri_f[b, at, :] = block[:, b * LANES : (b + 1) * LANES]
            return carry

        lax.fori_loop(0, peers, unpack, 0, unroll=4)

        def row(r, carry):
            t = jnp.concatenate(
                [tri_f[b, pl.ds(r, width, stride=rows), :] for b in range(blocks_per_half)], axis=1
            )
            mean = jnp.mean(t, axis=0, keepdims=True)
            centered = t - mean
            var = jnp.mean(centered * centered, axis=0, keepdims=True)
            scaled = centered * lax.rsqrt(var + EPSILON)
            gain = jnp.concatenate([gain_col[u]] * blocks_per_half, axis=1)
            update = dot((scaled * gain).astype(BF16), wo_ref[u], 0, 0)
            z = pair[r, there, :].astype(F32)
            result[r, there, :] = (z + update * gates[r, there, :]).astype(BF16)
            return carry

        lax.fori_loop(0, rows, row, 0)

    def each_member(action):
        def step(k, carry):
            at_offset = (offset + side + k) % length
            for cc in (other, core):
                for i in range(COLUMNS):
                    at_column = (column + i) % COLUMNS
                    may_be_self = i == 0 and cc is core
                    action(at_column, at_offset, cc, k == side if may_be_self else None)
            return carry

        lax.fori_loop(0, length, step, 0)

    def send_or_keep(from_ref, to_ref, ssem, rsem, at, own):
        if own is None:
            send(from_ref, to_ref, ssem, rsem, at)
            return

        @pl.when(jnp.logical_not(own))
        def _():
            send(from_ref, to_ref, ssem, rsem, at)

        @pl.when(own)
        def _():
            to_ref[...] = from_ref[...]

    def scatter(u, h, e, q):
        def one(at_column, at_offset, at_core, own):
            at_owner = (at_offset * COLUMNS + at_column) * 2 + at_core
            from_ref = src.at[u, h, e, at_owner]
            to_ref = land.at[u, h, e, mine]
            send_or_keep(
                from_ref if q is None else from_ref.at[q],
                to_ref if q is None else to_ref.at[q],
                scat_send.at[u, h, e],
                scat_recv.at[u, h, e],
                device(at_column, length * block + at_offset, at_core),
                own,
            )

        each_member(one)

    def return_tri(u, e, h):
        def one(at_column, at_offset, at_core, own):
            at_rows = origin(at_column, at_offset) * 2 + at_core
            send_or_keep(
                tri_out.at[u, h, e, at_rows],
                tri_in.at[u, h, e, owner],
                tri_send.at[u, h, e],
                tri_recv.at[u, h, e],
                device(at_column, length * block + at_offset, at_core),
                own,
            )

        each_member(one)

    def edges(u, first, number, z):
        project(u, first, number, z)
        h = first // blocks_per_half

        def pack(p, carry):
            for e in range(2):
                at = pl.ds(pl.multiple_of(p * tile + e * rows, rows), rows)
                for b in range(first, first + number):
                    for kind, store in ((0, right_f), (1, left_f)):
                        src[u, h, e, p, b % blocks_per_half, kind] = store[b, at, :].astype(BF16)
            return carry

        lax.fori_loop(0, peers, pack, 0, unroll=2)
        for e in range(2):
            scatter(u, h, e, None if number == blocks_per_half else first % blocks_per_half)

    def multiply(u, e):
        for h in range(2):
            ref = land.at[u, h, e, pl.ds(0, peers - 1)]
            waiter(ref, scat_send.at[0, 0, 0], scat_recv.at[u, h, e]).wait_recv()

        def split(s, carry):
            at = pl.ds(pl.multiple_of(s * tile, tile), tile)
            for kind, mat in ((1, mat_l), (0, mat_r)):
                for b in range(2 * blocks_per_half):
                    h, q = b // blocks_per_half, b % blocks_per_half
                    edge = land[u, h, e, pl.ds(2 * s, 2), q, kind].astype(F32)
                    mat[at, b * LANES : (b + 1) * LANES] = edge.reshape(tile, LANES).astype(BF16)
            return carry

        lax.fori_loop(0, chips, split, 0)
        some = peers // 2
        for b in range(2):
            for h in range(2):
                first, second = slice(b * cols, (b + 1) * cols), slice(h * cols, (h + 1) * cols)
                if u == 0:
                    product = dot(mat_l[first, :], mat_r[second, :], 1, 1)
                else:
                    product = dot(mat_l[:, first], mat_r[:, second], 0, 0)
                tri_out[u, h, e, b * some : (b + 1) * some] = product.reshape(
                    some, rows, cols
                ).astype(BF16)

    def triangle(u):
        multiply(u, 0)
        return_tri(u, 0, 0)
        multiply(u, 1)
        return_tri(u, 1, 0)
        return_tri(u, 0, 1)
        return_tri(u, 1, 1)

    def arrived(u, h):
        for e in range(2):
            ref = tri_in.at[u, h, e, pl.ds(0, peers - 1)]
            waiter(ref, tri_send.at[0, 0, 0], tri_recv.at[u, h, e]).wait_recv()

    per_half = parts // 2

    for f in range(parts):

        @pl.when(moves)
        def _():
            waiter(part(start_z, f), in_send.at[0], in_recv.at[f]).wait_recv()

        edges(0, f, 1, start_z)
    gate_values(0)
    triangle(0)

    for h in range(2):
        arrived(0, h)
        finish(0, h, start_z, middle)
        edges(1, h * blocks_per_half, blocks_per_half, middle)
    gate_values(1)
    triangle(1)

    far = from_chip != chip
    away = jnp.logical_and(far, column != block)
    near = jnp.logical_and(moves, jnp.logical_not(away))
    arrived(1, 0)
    finish(1, 0, middle, final_z)
    arrived(1, 1)

    def tell(k, carry):
        at = device(column, (chip + 1 + k) % chips, core)
        pl.semaphore_signal(calm, inc=1, device_id=at, device_id_type=MESH)
        return carry

    lax.fori_loop(0, chips - 1, tell, 0)
    finish(1, 1, middle, final_z)
    pl.semaphore_wait(calm, chips - 1)
    for h in range(2):
        for f in range(h * per_half, (h + 1) * per_half):

            @pl.when(away)
            def _():
                at = device(column, from_chip, core)
                held = relay_part(relay_out, block, f)
                send(part(final_z, f), held, out_send.at[f], out_relay_recv.at[block, f], at)

            @pl.when(near)
            def _():
                at = device(block, from_chip, core)
                send(part(final_z, f), part(home_z, f), out_send.at[f], out_recv.at[f], at)

    for f in range(parts):

        def pass_out(b, at_chip):
            held = relay_part(relay_out, b, f)
            waiter(held, out_send.at[0], out_relay_recv.at[b, f]).wait_recv()
            at = device(b, chip, core)
            send(held, part(home_z, f), out_relay_send.at[b, f], out_recv.at[f], at)

        each_relay(pass_out)

    for f in range(parts):
        there = pl.ds(f * part_cols, part_cols)

        @pl.when(moves)
        def _():
            waiter(part(home_z, f), out_send.at[0], out_recv.at[f]).wait_recv()
            out_ref[:, there, :] = home_z[:, there, :]

        @pl.when(stays)
        def _():
            out_ref[:, there, :] = final_z[:, there, :]

    @pl.when(block == column)
    def _():
        for i in range(1, COLUMNS):
            waiter(valid_own, valid_send.at[i - 1], valid_recv).wait_send()

    @pl.when(moves)
    def _():
        for f in range(parts):
            waiter(part(pair_ref, f), in_send.at[f], in_recv.at[f]).wait_send()
            waiter(part(final_z, f), out_send.at[f], out_recv.at[f]).wait_send()

    def left_relay(b, at_chip):
        for f in range(parts):
            waiter(relay_part(relay_in, b, f), in_relay_send.at[b, f], in_recv.at[f]).wait_send()
            waiter(relay_part(relay_out, b, f), out_relay_send.at[b, f], out_recv.at[f]).wait_send()

    each_relay(left_relay)
    for u in range(2):
        for h in range(2):
            for e in range(2):
                waiter(
                    src.at[u, h, e, pl.ds(0, peers - 1)], scat_send.at[u, h, e], scat_recv.at[u, h, e]
                ).wait_send()
                waiter(
                    tri_out.at[u, h, e, pl.ds(0, peers - 1)], tri_send.at[u, h, e], tri_recv.at[u, h, e]
                ).wait_send()


def per_device(peers, across, pair_in, valid_tokens, proj_weight, out_weight, norm_gains):
    rows, count, width = pair_in.shape
    cols = count // 2
    vmem = pltpu.VMEM
    dma = pltpu.SemaphoreType.DMA
    pair = vmem((rows, count, width), BF16)
    relayed = vmem((COLUMNS, rows, count, width), BF16)
    parts = count // LANES
    edge_tiles = vmem((2, 2, 2, peers, parts // 2, 2, rows, LANES), BF16)
    tri_tiles = vmem((2, 2, 2, peers, rows, cols), BF16)
    whole = pl.BlockSpec(memory_space=pltpu.VMEM)
    return pl.pallas_call(
        functools.partial(kernel, peers, across),
        out_shape=jax.ShapeDtypeStruct((rows, count, width), BF16),
        in_specs=[whole] * 5,
        out_specs=whole,
        scratch_shapes=[
            vmem((2, 4 * width, width), BF16),
            vmem((2, width, width), F32),
            vmem((count // LANES, width * rows, LANES), F32),
            vmem((count // LANES, width * rows, LANES), F32),
            vmem((cols // LANES, width * rows, LANES), F32),
            pair,
            vmem((rows, count, width), F32),
            vmem((8, count), F32),
            vmem((8, count), F32),
            pair,
            pair,
            pair,
            pair,
            relayed,
            relayed,
            edge_tiles,
            edge_tiles,
            vmem((count, count), BF16),
            vmem((count, count), BF16),
            tri_tiles,
            tri_tiles,
            dma((COLUMNS - 1,)),
            dma,
            dma((parts,)),
            dma((parts,)),
            dma((COLUMNS, parts)),
            dma((COLUMNS, parts)),
            dma((parts,)),
            dma((parts,)),
            dma((COLUMNS, parts)),
            dma((COLUMNS, parts)),
            dma((2, 2, 2)),
            dma((2, 2, 2)),
            dma((2, 2, 2)),
            dma((2, 2, 2)),
            pltpu.SemaphoreType.REGULAR,
        ],
        compiler_params=pltpu.CompilerParams(
            collective_id=0, has_side_effects=True, vmem_limit_bytes=60 * 1024 * 1024
        ),
    )(pair_in, valid_tokens.reshape(1, count), proj_weight, out_weight, norm_gains)


def solution(mesh):
    across = len({d.coords[0] for d in mesh.devices[:, 0]})
    return jax.shard_map(
        functools.partial(per_device, mesh.shape["row"], across),
        mesh=mesh,
        in_specs=(P(("groups", "row"), None, None), P("groups"), P(), P(), P()),
        out_specs=P(("groups", "row"), None, None),
        check_vma=False,
    )
```

```python
import functools

import jax
import jax.numpy as jnp
from jax import lax
from jax.experimental import pallas as pl
from jax.experimental.pallas import tpu as pltpu
from jax.sharding import PartitionSpec as P

MESH = pl.DeviceIdType.MESH
EPSILON = 1e-05
COLUMNS = 4
LANES = 128
BF16 = jnp.bfloat16
F32 = jnp.float32


def dot(a, b, contract_a, contract_b):
    return lax.dot_general(
        a, b, (((contract_a,), (contract_b,)), ((), ())), preferred_element_type=F32
    )


def kernel(
    peers,
    across,
    pair_ref,
    valid_ref,
    proj_ref,
    wo_ref,
    gain_ref,
    out_ref,
    wt,
    gain_col,
    left_f,
    right_f,
    tri_f,
    normed,
    gates,
    valid_own,
    valid_got,
    start_z,
    middle,
    final_z,
    home_z,
    relay_in,
    relay_out,
    src,
    land,
    mat_l,
    mat_r,
    tri_out,
    tri_in,
    valid_send,
    valid_recv,
    in_send,
    in_recv,
    in_relay_send,
    in_relay_recv,
    out_send,
    out_recv,
    out_relay_send,
    out_relay_recv,
    scat_send,
    scat_recv,
    tri_send,
    tri_recv,
    calm,
):
    rows, count, width = pair_ref.shape
    chips = peers // 2
    length = chips // COLUMNS
    side = length // 2
    outer = (chips - length) // 2
    cols = count // 2
    part_cols = LANES
    parts = count // LANES
    blocks_per_half = cols // LANES
    tile = 2 * rows
    me = lax.axis_index("row")
    chip = me // 2
    core = me % 2
    other = 1 - core
    group = lax.axis_index("groups")
    down = (group // across) % 2
    right = (group % across) % 2
    column = 2 * down + right
    block = chip // length
    offset = chip % length

    def device(at_column, at_chip, at_core):
        at_group = group + (at_column // 2 - down) * across + (at_column % 2 - right)
        return {"groups": at_group, "row": at_chip * 2 + at_core}

    def copier(from_ref, to_ref, ssem, rsem, at):
        return pltpu.make_async_remote_copy(
            src_ref=from_ref,
            dst_ref=to_ref,
            send_sem=ssem,
            recv_sem=rsem,
            device_id=at,
            device_id_type=MESH,
        )

    def send(from_ref, to_ref, ssem, rsem, at):
        copier(from_ref, to_ref, ssem, rsem, at).start()

    def waiter(ref, ssem, rsem):
        return copier(ref, ref, ssem, rsem, device(column, chip, other))

    def mirror(half, value):
        return value + half * (length - 1 - 2 * value)

    def placed(at_chip, of_group):
        t = (at_chip - length * of_group + outer + chips) % chips - outer
        half = (t + outer) // (2 * length)
        a = mirror(half, t) + outer
        turn = a % COLUMNS
        w = (turn + 1 + a // COLUMNS) % COLUMNS
        return (turn + of_group) % COLUMNS, length * of_group + mirror(half, w)

    def origin(at_column, at_offset):
        half = at_offset // side
        w = mirror(half, at_offset)
        turn = (at_column - block + COLUMNS) % COLUMNS
        k = (w - turn - 1 + 2 * COLUMNS) % COLUMNS
        t = mirror(half, COLUMNS * k + turn - outer)
        return (length * block + t + chips) % chips

    to_column, to_chip = placed(chip, column)
    from_chip = origin(column, offset)
    mine = from_chip * 2 + core
    owner = (offset * COLUMNS + column) * 2 + core
    stays = jnp.logical_and(to_column == column, to_chip == chip)
    moves = jnp.logical_not(stays)

    barrier = pltpu.get_barrier_semaphore()

    def greet_block(k, carry):
        at_chip = length * block + (offset + k) % length
        for i in range(COLUMNS):
            at_column = (column + i) % COLUMNS
            at = device(at_column, at_chip, other)
            pl.semaphore_signal(barrier, inc=1, device_id=at, device_id_type=MESH)
            at = device(at_column, at_chip, core)
            if i == 0:

                @pl.when(k != 0)
                def _():
                    pl.semaphore_signal(barrier, inc=1, device_id=at, device_id_type=MESH)
            else:
                pl.semaphore_signal(barrier, inc=1, device_id=at, device_id_type=MESH)
        return carry

    lax.fori_loop(0, length, greet_block, 0)

    def greet_column(k, carry):
        at = device(column, (length * (block + 1) + k) % chips, core)
        pl.semaphore_signal(barrier, inc=1, device_id=at, device_id_type=MESH)
        return carry

    lax.fori_loop(0, chips - length, greet_column, 0)

    valid_own[...] = jnp.broadcast_to(valid_ref[...].astype(F32), valid_own.shape)

    for u in range(2):
        for k in range(4):
            at = slice(k * width, (k + 1) * width)
            wt[u, at, :] = jnp.transpose(proj_ref[u, :, at].astype(F32)).astype(BF16)
        gain_col[u] = jnp.transpose(jnp.broadcast_to(gain_ref[u, 1:2, :], (width, width)))

    pl.semaphore_wait(barrier, 2 * COLUMNS * length - 1 + chips - length)

    def part(ref, f):
        return ref.at[:, pl.ds(f * part_cols, part_cols), :]

    two_steps = jnp.logical_and(to_column != column, to_chip != chip)
    one_step = jnp.logical_and(moves, jnp.logical_not(two_steps))

    @pl.when(block == column)
    def _():
        for i in range(1, COLUMNS):
            at = device((column + i) % COLUMNS, chip, core)
            send(valid_own, valid_got, valid_send.at[i - 1], valid_recv, at)
        valid_got[...] = valid_own[...]

    for f in range(parts):

        @pl.when(two_steps)
        def _():
            at = device(to_column, chip, core)
            dst = relay_in.at[column, :, pl.ds(f * part_cols, part_cols), :]
            send(part(pair_ref, f), dst, in_send.at[f], in_relay_recv.at[column, f], at)

        @pl.when(one_step)
        def _():
            at = device(to_column, to_chip, core)
            send(part(pair_ref, f), part(start_z, f), in_send.at[f], in_recv.at[f], at)

    @pl.when(stays)
    def _():
        start_z[...] = pair_ref[...]

    def each_relay(action):
        for b in range(COLUMNS):
            at_column, at_chip = placed(chip, b)
            here = jnp.logical_and(at_column == column, at_chip != chip)
            pl.when(jnp.logical_and(here, column != b))(functools.partial(action, b, at_chip))

    def relay_part(ref, b, f):
        return ref.at[b, :, pl.ds(f * part_cols, part_cols), :]

    for f in range(parts):

        def pass_in(b, at_chip):
            held = relay_part(relay_in, b, f)
            waiter(held, in_send.at[0], in_relay_recv.at[b, f]).wait_recv()
            at = device(column, at_chip, core)
            send(held, part(start_z, f), in_relay_send.at[b, f], in_recv.at[f], at)

        each_relay(pass_in)

    @pl.when(block != column)
    def _():
        waiter(valid_got, valid_send.at[0], valid_recv).wait_recv()

    def project(u, first, number, pair):
        there = pl.ds(first * LANES, number * LANES)
        valid = valid_got[0:1, first * LANES : (first + number) * LANES]
        token = lax.broadcasted_iota(jnp.int32, (1, count), 1)

        def row(r, carry):
            z = pair[r, there, :].astype(F32)
            mean = jnp.mean(z, axis=1, keepdims=True)
            centered = z - mean
            var = jnp.mean(centered * centered, axis=1, keepdims=True)
            x = (centered * lax.rsqrt(var + EPSILON) * gain_ref[u, 0:1, :]).astype(BF16)
            normed[r, there, :] = x
            own = jnp.where(token == mine * rows + r, valid_got[0:1, :], 0.0)
            m = valid * jnp.sum(own, axis=1, keepdims=True)
            for k, store in ((2, right_f), (0, left_f)):
                gate = dot(wt[u, k * width : (k + 1) * width, :], x, 1, 1)
                value = dot(wt[u, (k + 1) * width : (k + 2) * width, :], x, 1, 1)
                edge = jax.nn.sigmoid(gate) * value * m
                for b in range(number):
                    store[first + b, pl.ds(r, width, stride=rows), :] = edge[
                        :, b * LANES : (b + 1) * LANES
                    ]
            return carry

        lax.fori_loop(0, rows, row, 0)

    def gate_values(u):
        def row(r, carry):
            gates[r] = jax.nn.sigmoid(dot(normed[r], proj_ref[u, :, 4 * width :], 1, 0))
            return carry

        lax.fori_loop(0, rows, row, 0)

    def finish(u, h, pair, result):
        there = pl.ds(h * cols, cols)

        def unpack(p, carry):
            for e in range(2):
                at = pl.ds(pl.multiple_of(p * tile + e * rows, rows), rows)
                block = tri_in[u, h, e, p].astype(F32)
                for b in range(blocks_per_half):
                    tri_f[b, at, :] = block[:, b * LANES : (b + 1) * LANES]
            return carry

        lax.fori_loop(0, peers, unpack, 0, unroll=4)

        def row(r, carry):
            t = jnp.concatenate(
                [tri_f[b, pl.ds(r, width, stride=rows), :] for b in range(blocks_per_half)], axis=1
            )
            mean = jnp.mean(t, axis=0, keepdims=True)
            centered = t - mean
            var = jnp.mean(centered * centered, axis=0, keepdims=True)
            scaled = centered * lax.rsqrt(var + EPSILON)
            gain = jnp.concatenate([gain_col[u]] * blocks_per_half, axis=1)
            update = dot((scaled * gain).astype(BF16), wo_ref[u], 0, 0)
            z = pair[r, there, :].astype(F32)
            result[r, there, :] = (z + update * gates[r, there, :]).astype(BF16)
            return carry

        lax.fori_loop(0, rows, row, 0)

    def each_member(action):
        def step(k, carry):
            at_offset = (offset + side + k) % length
            for cc in (other, core):
                for i in range(COLUMNS):
                    at_column = (column + i) % COLUMNS
                    may_be_self = i == 0 and cc is core
                    action(at_column, at_offset, cc, k == side if may_be_self else None)
            return carry

        lax.fori_loop(0, length, step, 0)

    def send_or_keep(from_ref, to_ref, ssem, rsem, at, own):
        if own is None:
            send(from_ref, to_ref, ssem, rsem, at)
            return

        @pl.when(jnp.logical_not(own))
        def _():
            send(from_ref, to_ref, ssem, rsem, at)

        @pl.when(own)
        def _():
            to_ref[...] = from_ref[...]

    def scatter(u, h, e, q):
        def one(at_column, at_offset, at_core, own):
            at_owner = (at_offset * COLUMNS + at_column) * 2 + at_core
            from_ref = src.at[u, h, e, at_owner]
            to_ref = land.at[u, h, e, mine]
            send_or_keep(
                from_ref if q is None else from_ref.at[q],
                to_ref if q is None else to_ref.at[q],
                scat_send.at[u, h, e],
                scat_recv.at[u, h, e],
                device(at_column, length * block + at_offset, at_core),
                own,
            )

        each_member(one)

    def return_tri(u, e, h):
        def one(at_column, at_offset, at_core, own):
            at_rows = origin(at_column, at_offset) * 2 + at_core
            send_or_keep(
                tri_out.at[u, h, e, at_rows],
                tri_in.at[u, h, e, owner],
                tri_send.at[u, h, e],
                tri_recv.at[u, h, e],
                device(at_column, length * block + at_offset, at_core),
                own,
            )

        each_member(one)

    def edges(u, first, number, z):
        project(u, first, number, z)
        h = first // blocks_per_half

        def pack(p, carry):
            for e in range(2):
                at = pl.ds(pl.multiple_of(p * tile + e * rows, rows), rows)
                for b in range(first, first + number):
                    for kind, store in ((0, right_f), (1, left_f)):
                        src[u, h, e, p, b % blocks_per_half, kind] = store[b, at, :].astype(BF16)
            return carry

        lax.fori_loop(0, peers, pack, 0, unroll=2)
        for e in range(2):
            scatter(u, h, e, None if number == blocks_per_half else first % blocks_per_half)

    def multiply(u, e):
        for h in range(2):
            ref = land.at[u, h, e, pl.ds(0, peers - 1)]
            waiter(ref, scat_send.at[0, 0, 0], scat_recv.at[u, h, e]).wait_recv()

        def split(s, carry):
            at = pl.ds(pl.multiple_of(s * tile, tile), tile)
            for kind, mat in ((1, mat_l), (0, mat_r)):
                for b in range(2 * blocks_per_half):
                    h, q = b // blocks_per_half, b % blocks_per_half
                    edge = land[u, h, e, pl.ds(2 * s, 2), q, kind].astype(F32)
                    mat[at, b * LANES : (b + 1) * LANES] = edge.reshape(tile, LANES).astype(BF16)
            return carry

        lax.fori_loop(0, chips, split, 0)
        some = peers // 2
        for b in range(2):
            for h in range(2):
                first, second = slice(b * cols, (b + 1) * cols), slice(h * cols, (h + 1) * cols)
                if u == 0:
                    product = dot(mat_l[first, :], mat_r[second, :], 1, 1)
                else:
                    product = dot(mat_l[:, first], mat_r[:, second], 0, 0)
                tri_out[u, h, e, b * some : (b + 1) * some] = product.reshape(
                    some, rows, cols
                ).astype(BF16)

    def triangle(u):
        multiply(u, 0)
        return_tri(u, 0, 0)
        multiply(u, 1)
        return_tri(u, 1, 0)
        return_tri(u, 0, 1)
        return_tri(u, 1, 1)

    def arrived(u, h):
        for e in range(2):
            ref = tri_in.at[u, h, e, pl.ds(0, peers - 1)]
            waiter(ref, tri_send.at[0, 0, 0], tri_recv.at[u, h, e]).wait_recv()

    per_half = parts // 2

    for f in range(parts):

        @pl.when(moves)
        def _():
            waiter(part(start_z, f), in_send.at[0], in_recv.at[f]).wait_recv()

        edges(0, f, 1, start_z)
    gate_values(0)
    triangle(0)

    for h in range(2):
        arrived(0, h)
        finish(0, h, start_z, middle)
        edges(1, h * blocks_per_half, blocks_per_half, middle)
    gate_values(1)
    triangle(1)

    far = from_chip != chip
    away = jnp.logical_and(far, column != block)
    near = jnp.logical_and(moves, jnp.logical_not(away))
    arrived(1, 0)

    def tell(k, carry):
        at = device(column, (chip + 1 + k) % chips, core)
        pl.semaphore_signal(calm, inc=1, device_id=at, device_id_type=MESH)
        return carry

    lax.fori_loop(0, chips - 1, tell, 0)
    finish(1, 0, middle, final_z)
    arrived(1, 1)
    finish(1, 1, middle, final_z)
    pl.semaphore_wait(calm, chips - 1)
    for h in range(2):
        for f in range(h * per_half, (h + 1) * per_half):

            @pl.when(away)
            def _():
                at = device(column, from_chip, core)
                held = relay_part(relay_out, block, f)
                send(part(final_z, f), held, out_send.at[f], out_relay_recv.at[block, f], at)

            @pl.when(near)
            def _():
                at = device(block, from_chip, core)
                send(part(final_z, f), part(home_z, f), out_send.at[f], out_recv.at[f], at)

    for f in range(parts):

        def pass_out(b, at_chip):
            held = relay_part(relay_out, b, f)
            waiter(held, out_send.at[0], out_relay_recv.at[b, f]).wait_recv()
            at = device(b, chip, core)
            send(held, part(home_z, f), out_relay_send.at[b, f], out_recv.at[f], at)

        each_relay(pass_out)

    for f in range(parts):
        there = pl.ds(f * part_cols, part_cols)

        @pl.when(moves)
        def _():
            waiter(part(home_z, f), out_send.at[0], out_recv.at[f]).wait_recv()
            out_ref[:, there, :] = home_z[:, there, :]

        @pl.when(stays)
        def _():
            out_ref[:, there, :] = final_z[:, there, :]

    @pl.when(block == column)
    def _():
        for i in range(1, COLUMNS):
            waiter(valid_own, valid_send.at[i - 1], valid_recv).wait_send()

    @pl.when(moves)
    def _():
        for f in range(parts):
            waiter(part(pair_ref, f), in_send.at[f], in_recv.at[f]).wait_send()
            waiter(part(final_z, f), out_send.at[f], out_recv.at[f]).wait_send()

    def left_relay(b, at_chip):
        for f in range(parts):
            waiter(relay_part(relay_in, b, f), in_relay_send.at[b, f], in_recv.at[f]).wait_send()
            waiter(relay_part(relay_out, b, f), out_relay_send.at[b, f], out_recv.at[f]).wait_send()

    each_relay(left_relay)
    for u in range(2):
        for h in range(2):
            for e in range(2):
                waiter(
                    src.at[u, h, e, pl.ds(0, peers - 1)], scat_send.at[u, h, e], scat_recv.at[u, h, e]
                ).wait_send()
                waiter(
                    tri_out.at[u, h, e, pl.ds(0, peers - 1)], tri_send.at[u, h, e], tri_recv.at[u, h, e]
                ).wait_send()


def per_device(peers, across, pair_in, valid_tokens, proj_weight, out_weight, norm_gains):
    rows, count, width = pair_in.shape
    cols = count // 2
    vmem = pltpu.VMEM
    dma = pltpu.SemaphoreType.DMA
    pair = vmem((rows, count, width), BF16)
    relayed = vmem((COLUMNS, rows, count, width), BF16)
    parts = count // LANES
    edge_tiles = vmem((2, 2, 2, peers, parts // 2, 2, rows, LANES), BF16)
    tri_tiles = vmem((2, 2, 2, peers, rows, cols), BF16)
    whole = pl.BlockSpec(memory_space=pltpu.VMEM)
    return pl.pallas_call(
        functools.partial(kernel, peers, across),
        out_shape=jax.ShapeDtypeStruct((rows, count, width), BF16),
        in_specs=[whole] * 5,
        out_specs=whole,
        scratch_shapes=[
            vmem((2, 4 * width, width), BF16),
            vmem((2, width, width), F32),
            vmem((count // LANES, width * rows, LANES), F32),
            vmem((count // LANES, width * rows, LANES), F32),
            vmem((cols // LANES, width * rows, LANES), F32),
            pair,
            vmem((rows, count, width), F32),
            vmem((8, count), F32),
            vmem((8, count), F32),
            pair,
            pair,
            pair,
            pair,
            relayed,
            relayed,
            edge_tiles,
            edge_tiles,
            vmem((count, count), BF16),
            vmem((count, count), BF16),
            tri_tiles,
            tri_tiles,
            dma((COLUMNS - 1,)),
            dma,
            dma((parts,)),
            dma((parts,)),
            dma((COLUMNS, parts)),
            dma((COLUMNS, parts)),
            dma((parts,)),
            dma((parts,)),
            dma((COLUMNS, parts)),
            dma((COLUMNS, parts)),
            dma((2, 2, 2)),
            dma((2, 2, 2)),
            dma((2, 2, 2)),
            dma((2, 2, 2)),
            pltpu.SemaphoreType.REGULAR,
        ],
        compiler_params=pltpu.CompilerParams(
            collective_id=0, has_side_effects=True, vmem_limit_bytes=60 * 1024 * 1024
        ),
    )(pair_in, valid_tokens.reshape(1, count), proj_weight, out_weight, norm_gains)


def solution(mesh):
    across = len({d.coords[0] for d in mesh.devices[:, 0]})
    return jax.shard_map(
        functools.partial(per_device, mesh.shape["row"], across),
        mesh=mesh,
        in_specs=(P(("groups", "row"), None, None), P("groups"), P(), P(), P()),
        out_specs=P(("groups", "row"), None, None),
        check_vma=False,
    )
```
